32 devices in a mesh: dp: 4 (over y, z), ep: 8 (over x, core).
Axes of the slice: x: 4, y: 2, z: 2, core: 2. Of those that a mesh axis runs over, the one named last changes fastest.
The devices are a block of a 4x4x8 slice.
Arguments:
- x_tok: bfloat16 [32, 512, 2048], P(('dp', 'ep')), parts along dimension 0
- w_query: bfloat16 [2048, 16, 128], P('ep')
- w_key: bfloat16 [2048, 16, 128], P('ep')
- w_value: bfloat16 [2048, 16, 128], P('ep')
- w_out: bfloat16 [2048, 2048], P('ep')
- w_router: float32 [2048, 64], replicated
- w_gate: bfloat16 [64, 2048, 1024], P('ep')
- w_up: bfloat16 [64, 2048, 1024], P('ep')
- w_down: bfloat16 [64, 1024, 2048], P('ep')
- ws_gate: bfloat16 [2048, 1024], P('ep')
- ws_up: bfloat16 [2048, 1024], P('ep')
- ws_down: bfloat16 [1024, 2048], P('ep')
- expert_ids: int32 [32, 512, 8], P(('dp', 'ep')), parts along dimension 0
Outputs:
- output: bfloat16 [32, 512, 2048], P(('dp', 'ep')), parts along dimension 0
There are 4 independent parts. The reference program is written for one: setup_inputs(seed, part) draws one part's arguments, and reference() takes and returns one part's arrays. A program takes and returns all parts, laid end to end along the dimension named above; an argument that names none is the same for every part.
All inputs are finite; a program needn't handle non-finite values.
Results may differ from the reference program's by a relative error of at most 0.0133186.
Values are sent between devices in bfloat16 or wider.
A program may use at most 768 MiB of HBM per device.

```python
import jax
import jax.numpy as jnp
import numpy as np
from jax import lax

SEQS_DEV = 1
SEQ = 512
GROUP = 8
D = 2048
HEADS = 16
HEAD = 128
EXPERTS = 64
TOP = 8
FF = 1024
FFS = 1024
CAP = 128
NHOT = 8

EPSILON = 1e-6
TOK_DEV = SEQS_DEV * SEQ
TOKENS = GROUP * TOK_DEV
N_SEQS = GROUP * SEQS_DEV
WIDTH = HEADS * HEAD


def rms_norm(values):
    as_f32 = values.astype(jnp.float32)
    return as_f32 * lax.rsqrt(jnp.mean(as_f32 * as_f32, axis=-1, keepdims=True) + EPSILON)


def swiglu_ffn(row_block, gate_w, up_w, down_w):
    gate_act = jnp.dot(row_block, gate_w, preferred_element_type=jnp.float32)
    up_act = jnp.dot(row_block, up_w, preferred_element_type=jnp.float32)
    middle = (jax.nn.silu(gate_act) * up_act).astype(jnp.bfloat16)
    return jnp.dot(middle, down_w, preferred_element_type=jnp.float32).astype(jnp.bfloat16)


def routing_table():
    rest_count = TOK_DEV * TOP - NHOT * CAP
    cold_count = EXPERTS - NHOT
    run_counts = np.concatenate([np.full(NHOT, CAP), rest_count // cold_count + (np.arange(cold_count) < rest_count % cold_count)])
    return jnp.asarray(np.repeat(np.arange(EXPERTS), run_counts), dtype=jnp.int32)


def device_routing(dev_key, run_ids):
    label_key, order_key = jax.random.split(dev_key)
    labels = jax.random.permutation(label_key, EXPERTS)
    shuffle = jax.random.permutation(order_key, TOK_DEV)
    table = labels[run_ids].reshape(TOP, TOK_DEV).T
    return table[shuffle]


def setup_inputs(seed: int = 0, part: int = 0) -> dict:
    root_key = jax.random.key(seed)
    part_key = jax.random.fold_in(root_key, part)
    tok_key, route_key = jax.random.split(part_key)
    weight_keys = jax.random.split(root_key, 10)

    def gauss(key_w, shape_w, scale):
        return (jax.random.normal(key_w, shape_w, jnp.float32) * scale).astype(jnp.bfloat16)

    run_ids = routing_table()

    def draw_device(dev_key):
        return device_routing(dev_key, run_ids)

    dev_keys = jax.random.split(route_key, GROUP)
    expert_ids = jax.vmap(draw_device)(dev_keys).reshape(N_SEQS, SEQ, TOP)
    return {
        'x_tok': jax.random.normal(tok_key, (N_SEQS, SEQ, D), jnp.float32).astype(jnp.bfloat16),
        'w_query': gauss(weight_keys[0], (D, HEADS, HEAD), 2.0 * D ** -0.5),
        'w_key': gauss(weight_keys[1], (D, HEADS, HEAD), D ** -0.5),
        'w_value': gauss(weight_keys[2], (D, HEADS, HEAD), D ** -0.5),
        'w_out': gauss(weight_keys[3], (WIDTH, D), 2.0 * WIDTH ** -0.5),
        'w_router': jax.random.normal(weight_keys[4], (D, EXPERTS), jnp.float32) * D ** -0.5,
        'w_gate': gauss(weight_keys[5], (EXPERTS, D, FF), D ** -0.5),
        'w_up': gauss(weight_keys[6], (EXPERTS, D, FF), D ** -0.5),
        'w_down': gauss(weight_keys[7], (EXPERTS, FF, D), 2.0 * FF ** -0.5),
        'ws_gate': gauss(weight_keys[8], (D, FFS), D ** -0.5),
        'ws_up': gauss(weight_keys[9], (D, FFS), D ** -0.5),
        'ws_down': gauss(jax.random.fold_in(root_key, 11), (FFS, D), FFS ** -0.5),
        'expert_ids': expert_ids,
    }


def reference(x_tok, w_query, w_key, w_value, w_out, w_router, w_gate, w_up, w_down, ws_gate, ws_up, ws_down, expert_ids):
    normed = rms_norm(x_tok).astype(jnp.bfloat16).reshape(TOKENS, D)

    def project(weight):
        return jnp.dot(normed, weight.reshape(D, WIDTH), preferred_element_type=jnp.float32).astype(jnp.bfloat16).reshape(N_SEQS, SEQ, HEADS, HEAD)

    queries = project(w_query)
    keys_all = project(w_key)
    vals_all = project(w_value)
    causal = jnp.arange(SEQ)[:, None] >= jnp.arange(SEQ)[None, :]

    def one_seq(seq_block):
        query_blk, key_blk, value_blk = seq_block
        scores = jnp.einsum('qhe,khe->hqk', query_blk.astype(jnp.float32), key_blk.astype(jnp.float32)) * (HEAD ** -0.5)
        attn_probs = jax.nn.softmax(jnp.where(causal[None], scores, -1e30), axis=-1).astype(jnp.bfloat16)
        return jnp.einsum('hqk,khe->qhe', attn_probs.astype(jnp.float32), value_blk.astype(jnp.float32)).astype(jnp.bfloat16)

    attended = lax.map(one_seq, (queries, keys_all, vals_all))
    attn_out = jnp.dot(attended.reshape(TOKENS, WIDTH), w_out, preferred_element_type=jnp.float32).astype(jnp.bfloat16)
    residual = (x_tok.reshape(TOKENS, D).astype(jnp.float32) + attn_out.astype(jnp.float32)).astype(jnp.bfloat16)

    hidden = rms_norm(residual)
    logits = jnp.dot(hidden, w_router, preferred_element_type=jnp.float32)
    tok_ids = expert_ids.reshape(TOKENS, TOP)
    gate_probs = jax.nn.softmax(jnp.take_along_axis(logits, tok_ids, axis=1), axis=-1)
    moe_in = hidden.astype(jnp.bfloat16)

    flat_ids = tok_ids.reshape(-1)
    n_assign = TOKENS * TOP
    sort_order = jnp.argsort(flat_ids, stable=True)
    expert_counts = jnp.bincount(flat_ids, length=EXPERTS)
    expert_starts = jnp.cumsum(expert_counts) - expert_counts
    slot_count = GROUP * CAP
    flat_gates = gate_probs.reshape(-1)

    def one_expert(running, piece):
        gate_w, up_w, down_w, start_at, count_of = piece
        slot_picks = jnp.minimum(start_at + jnp.arange(slot_count), n_assign - 1)
        assign_ids = sort_order[slot_picks]
        slot_gate = jnp.where(jnp.arange(slot_count) < count_of, flat_gates[assign_ids], 0.0)
        slot_token = assign_ids // TOP
        outputs = swiglu_ffn(moe_in[slot_token], gate_w, up_w, down_w)
        running = running.at[slot_token].add(slot_gate[:, None] * outputs.astype(jnp.float32))
        return running, None

    routed, unused = lax.scan(one_expert, jnp.zeros((TOKENS, D), jnp.float32), (w_gate, w_up, w_down, expert_starts, expert_counts))
    shared = swiglu_ffn(moe_in, ws_gate, ws_up, ws_down)
    y_out = (residual.astype(jnp.float32) + routed + shared.astype(jnp.float32)).astype(jnp.bfloat16)
    return y_out.reshape(N_SEQS, SEQ, D)
```

```python
import functools
import jax
import jax.numpy as jnp
from jax import lax
from jax.experimental import pallas as pl
from jax.experimental.pallas import tpu as pltpu
from jax.sharding import PartitionSpec as P

EPSILON = 1e-6
CAP_FACTOR = 2
VMEM_BYTES = 60 * 1024 * 1024


def rms_norm(values):
    as_f32 = values.astype(jnp.float32)
    return as_f32 * lax.rsqrt(jnp.mean(as_f32 * as_f32, axis=-1, keepdims=True) + EPSILON)


def params(**kw):
    return pltpu.CompilerParams(vmem_limit_bytes=VMEM_BYTES, **kw)


def attention_kernel(q_ref, k_ref, v_ref, o_ref, *, parts):
    seq, head = q_ref.shape
    step = seq // parts
    for part in range(parts):
        lo, hi = part * step, (part + 1) * step
        scores = lax.dot_general(q_ref[lo:hi, :], k_ref[:hi, :], (((1,), (1,)), ((), ())), preferred_element_type=jnp.float32) * (head ** -0.5)
        rows = lo + lax.broadcasted_iota(jnp.int32, scores.shape, 0)
        cols = lax.broadcasted_iota(jnp.int32, scores.shape, 1)
        scores = jnp.where(rows >= cols, scores, -1e30)
        weights = jnp.exp(scores - jnp.max(scores, axis=-1, keepdims=True))
        probs = (weights / jnp.sum(weights, axis=-1, keepdims=True)).astype(jnp.bfloat16)
        o_ref[lo:hi, :] = jnp.dot(probs, v_ref[:hi, :], preferred_element_type=jnp.float32).astype(jnp.bfloat16)


def attention(queries, keys, vals, head):
    seq, width = queries.shape
    spec = pl.BlockSpec((seq, head), lambda i: (0, i))
    return pl.pallas_call(
        functools.partial(attention_kernel, parts=2),
        grid=(width // head,),
        in_specs=[spec] * 3,
        out_specs=spec,
        out_shape=jax.ShapeDtypeStruct((seq, width), jnp.bfloat16),
        compiler_params=params(),
        cost_estimate=pl.CostEstimate(flops=8 * seq * seq * width, bytes_accessed=8 * seq * width, transcendentals=0),
        name="attention",
    )(queries, keys, vals)


def dispatch_kernel(rank_ref, u_ref, x_ref, *, capacity):
    local = rank_ref.shape[1]
    n_tok = u_ref.shape[1]
    picks = []
    slots = lax.broadcasted_iota(jnp.int32, (capacity, n_tok), 0)
    for e in range(local):
        picks.append((rank_ref[0, e:e + 1, :] == slots).astype(jnp.float32).astype(jnp.bfloat16))
    pick = jnp.concatenate(picks, axis=0)
    width = 512
    for c in range(u_ref.shape[2] // width):
        cols = slice(c * width, (c + 1) * width)
        rows = jnp.dot(pick, u_ref[0, :, cols], preferred_element_type=jnp.float32).astype(jnp.bfloat16)
        for e in range(local):
            x_ref[e, 0, :, cols] = rows[e * capacity:(e + 1) * capacity, :]


def dispatch(rank, tokens, capacity):
    n_src, local, n_tok = rank.shape
    d_model = tokens.shape[2]
    return pl.pallas_call(
        functools.partial(dispatch_kernel, capacity=capacity),
        grid=(n_src,),
        in_specs=[pl.BlockSpec((1, local, n_tok), lambda s: (s, 0, 0)), pl.BlockSpec((1, n_tok, d_model), lambda s: (s, 0, 0))],
        out_specs=pl.BlockSpec((local, 1, capacity, d_model), lambda s: (0, s, 0, 0)),
        out_shape=jax.ShapeDtypeStruct((local, n_src, capacity, d_model), jnp.bfloat16),
        compiler_params=params(),
        cost_estimate=pl.CostEstimate(flops=2 * n_src * local * capacity * n_tok * d_model, bytes_accessed=4 * n_src * local * capacity * d_model, transcendentals=0),
        name="dispatch",
    )(rank, tokens)


def expert_kernel(x_ref, gate_ref, up_ref, down_ref, f_ref, *, chunk):
    n_rows = x_ref.shape[1]

    @pl.loop(0, n_rows // chunk)
    def _(i):
        rows = pl.ds(pl.multiple_of(i * chunk, chunk), chunk)
        x = x_ref[0, rows, :]
        gate_act = jnp.dot(x, gate_ref[0], preferred_element_type=jnp.float32)
        up_act = jnp.dot(x, up_ref[0], preferred_element_type=jnp.float32)
        middle = (gate_act * jax.nn.sigmoid(gate_act) * up_act).astype(jnp.bfloat16)
        f_ref[0, rows, :] = jnp.dot(middle, down_ref[0], preferred_element_type=jnp.float32).astype(jnp.bfloat16)


def experts(rows, gate_w, up_w, down_w):
    local, n_rows, d_model = rows.shape
    width = gate_w.shape[2]
    return pl.pallas_call(
        functools.partial(expert_kernel, chunk=256),
        grid=(local,),
        in_specs=[
            pl.BlockSpec((1, n_rows, d_model), lambda e: (e, 0, 0)),
            pl.BlockSpec((1, d_model, width), lambda e: (e, 0, 0)),
            pl.BlockSpec((1, d_model, width), lambda e: (e, 0, 0)),
            pl.BlockSpec((1, width, d_model), lambda e: (e, 0, 0)),
        ],
        out_specs=pl.BlockSpec((1, n_rows, d_model), lambda e: (e, 0, 0)),
        out_shape=jax.ShapeDtypeStruct(rows.shape, jnp.bfloat16),
        compiler_params=params(),
        cost_estimate=pl.CostEstimate(flops=6 * local * n_rows * d_model * width, bytes_accessed=6 * local * d_model * width, transcendentals=0),
        name="experts",
    )(rows, gate_w, up_w, down_w)


def combine_kernel(rank_ref, piece_ref, f_ref, out_ref):
    n_tok, local = rank_ref.shape[1:]
    capacity = f_ref.shape[2]
    pieces = piece_ref.shape[2] // local
    slots = lax.broadcasted_iota(jnp.int32, (n_tok, capacity), 1)
    rank = rank_ref[0]
    weights = piece_ref[0]
    rows = [[] for _ in range(pieces)]
    for e in range(local):
        hit = rank[:, e:e + 1] == slots
        for k in range(pieces):
            column = k * local + e
            rows[k].append(jnp.where(hit, weights[:, column:column + 1], 0.0).astype(jnp.bfloat16))
    spread = [jnp.concatenate(r, axis=1) for r in rows]
    width = 512
    for c in range(out_ref.shape[2] // width):
        cols = slice(c * width, (c + 1) * width)
        data = jnp.concatenate([f_ref[e, 0, :, cols] for e in range(local)], axis=0)
        total = jnp.dot(spread[0], data, preferred_element_type=jnp.float32)
        for k in range(1, pieces):
            total += jnp.dot(spread[k], data, preferred_element_type=jnp.float32)
        out_ref[0, :, cols] = total


def combine(rank_t, pieces, results):
    local, n_src, capacity, d_model = results.shape
    n_tok = rank_t.shape[1]
    width = pieces.shape[2]
    return pl.pallas_call(
        combine_kernel,
        grid=(n_src,),
        in_specs=[
            pl.BlockSpec((1, n_tok, local), lambda s: (s, 0, 0)),
            pl.BlockSpec((1, n_tok, width), lambda s: (s, 0, 0)),
            pl.BlockSpec((local, 1, capacity, d_model), lambda s: (0, s, 0, 0)),
        ],
        out_specs=pl.BlockSpec((1, n_tok, d_model), lambda s: (s, 0, 0)),
        out_shape=jax.ShapeDtypeStruct((n_src, n_tok, d_model), jnp.float32),
        compiler_params=params(),
        cost_estimate=pl.CostEstimate(flops=6 * n_src * local * capacity * n_tok * d_model, bytes_accessed=8 * n_src * local * capacity * d_model, transcendentals=0),
        name="combine",
    )(rank_t, pieces, results)


def bf16_pieces(values):
    first = lax.reduce_precision(values, 8, 7)
    second = lax.reduce_precision(values - first, 8, 7)
    third = values - first - second
    return first, second, third


def local_layer(x_loc, q_shard, k_shard, v_shard, o_shard, w_router, gate_loc, up_loc, down_loc, sgate_shard, sup_shard, sdown_shard, ids_loc, group):
    n_seq, seq_len, d_model = x_loc.shape
    heads, head = q_shard.shape[1:]
    n_tok = n_seq * seq_len
    top_k = ids_loc.shape[-1]
    local = gate_loc.shape[0]
    n_experts = local * group
    capacity = CAP_FACTOR * n_tok * top_k // n_experts

    def gathered(shard):
        return lax.all_gather(shard.reshape(shard.shape[0], -1), 'ep', axis=0, tiled=True)

    def project(rows, weight):
        return jnp.dot(rows, weight, preferred_element_type=jnp.float32).astype(jnp.bfloat16)

    ids_all = lax.all_gather(ids_loc.reshape(n_tok, top_k).T, 'ep', axis=0)
    mine = lax.axis_index('ep') * local + jnp.arange(local)
    chosen = ids_all[:, None, :, :] == mine[None, :, None, None]
    member = jnp.any(chosen, axis=2)
    before = (jnp.arange(n_tok)[:, None] < jnp.arange(n_tok)[None, :]).astype(jnp.bfloat16)
    rank = jnp.einsum('set,tq->seq', member.astype(jnp.bfloat16), before, preferred_element_type=jnp.float32).astype(jnp.int32)
    rank = jnp.where(member, rank, -1)

    x_flat = x_loc.reshape(n_tok, d_model)
    normed = rms_norm(x_flat).astype(jnp.bfloat16)
    queries = project(normed, gathered(q_shard))
    keys_all = project(normed, gathered(k_shard))
    vals_all = project(normed, gathered(v_shard))
    attended = [attention(queries[i * seq_len:(i + 1) * seq_len], keys_all[i * seq_len:(i + 1) * seq_len], vals_all[i * seq_len:(i + 1) * seq_len], head) for i in range(n_seq)]
    attended = attended[0] if n_seq == 1 else jnp.concatenate(attended, axis=0)
    attn_out = project(attended, gathered(o_shard))
    residual = (x_flat.astype(jnp.float32) + attn_out.astype(jnp.float32)).astype(jnp.bfloat16)

    hidden = rms_norm(residual)
    moe_in = hidden.astype(jnp.bfloat16)
    tokens = lax.all_gather(moe_in, 'ep', axis=0)
    logits = jnp.dot(hidden, w_router, precision=lax.Precision.HIGHEST, preferred_element_type=jnp.float32)
    tok_ids = ids_loc.reshape(n_tok, top_k)
    picked = tok_ids[:, :, None] == jnp.arange(n_experts)[None, None, :]
    chosen_logits = jnp.sum(jnp.where(picked, logits[:, None, :], 0.0), axis=2)
    gate_probs = jax.nn.softmax(chosen_logits, axis=-1)
    gates_all = lax.all_gather(gate_probs.T, 'ep', axis=0)
    weight = jnp.sum(jnp.where(chosen, gates_all[:, None, :, :], 0.0), axis=2)
    pieces = jnp.concatenate(bf16_pieces(weight), axis=1).transpose(0, 2, 1)

    rows = dispatch(rank, tokens, capacity)
    results = experts(rows.reshape(local, group * capacity, d_model), gate_loc, up_loc, down_loc)
    partial = combine(rank.transpose(0, 2, 1), pieces, results.reshape(local, group, capacity, d_model))
    routed = lax.psum_scatter(partial.reshape(group * n_tok, d_model), 'ep', scatter_dimension=0, tiled=True)

    gate_act = jnp.dot(moe_in, gathered(sgate_shard), preferred_element_type=jnp.float32)
    up_act = jnp.dot(moe_in, gathered(sup_shard), preferred_element_type=jnp.float32)
    middle = (jax.nn.silu(gate_act) * up_act).astype(jnp.bfloat16)
    shared = project(middle, gathered(sdown_shard))
    y_out = (residual.astype(jnp.float32) + routed + shared.astype(jnp.float32)).astype(jnp.bfloat16)
    return y_out.reshape(n_seq, seq_len, d_model)


def solution(mesh):
    tok_spec = P(('dp', 'ep'), None, None)
    row_spec = P('ep', None)
    cube_spec = P('ep', None, None)
    in_specs = (tok_spec, cube_spec, cube_spec, cube_spec, row_spec, P(None, None), cube_spec, cube_spec, cube_spec, row_spec, row_spec, row_spec, tok_spec)
    return jax.shard_map(functools.partial(local_layer, group=mesh.shape['ep']), mesh=mesh, in_specs=in_specs, out_specs=tok_spec, check_vma=False)
```

```python
import functools
import jax
import jax.numpy as jnp
from jax import lax
from jax.experimental import pallas as pl
from jax.experimental.pallas import tpu as pltpu
from jax.sharding import PartitionSpec as P

EPSILON = 1e-6
CAP_FACTOR = 2
ALIGN = 16
VMEM_BYTES = 60 * 1024 * 1024


def rms_norm(values):
    as_f32 = values.astype(jnp.float32)
    return as_f32 * lax.rsqrt(jnp.mean(as_f32 * as_f32, axis=-1, keepdims=True) + EPSILON)


def params(**kw):
    return pltpu.CompilerParams(vmem_limit_bytes=VMEM_BYTES, **kw)


def attention_kernel(q_ref, k_ref, v_ref, o_ref, *, parts):
    seq, head = q_ref.shape
    step = seq // parts
    for part in range(parts):
        lo, hi = part * step, (part + 1) * step
        scores = lax.dot_general(q_ref[lo:hi, :], k_ref[:hi, :], (((1,), (1,)), ((), ())), preferred_element_type=jnp.float32) * (head ** -0.5)
        rows = lo + lax.broadcasted_iota(jnp.int32, scores.shape, 0)
        cols = lax.broadcasted_iota(jnp.int32, scores.shape, 1)
        scores = jnp.where(rows >= cols, scores, -1e30)
        weights = jnp.exp(scores - jnp.max(scores, axis=-1, keepdims=True))
        probs = (weights / jnp.sum(weights, axis=-1, keepdims=True)).astype(jnp.bfloat16)
        o_ref[lo:hi, :] = jnp.dot(probs, v_ref[:hi, :], preferred_element_type=jnp.float32).astype(jnp.bfloat16)


def attention(queries, keys, vals, head):
    seq, width = queries.shape
    spec = pl.BlockSpec((seq, head), lambda i: (0, i))
    return pl.pallas_call(
        functools.partial(attention_kernel, parts=2),
        grid=(width // head,),
        in_specs=[spec] * 3,
        out_specs=spec,
        out_shape=jax.ShapeDtypeStruct((seq, width), jnp.bfloat16),
        compiler_params=params(),
        cost_estimate=pl.CostEstimate(flops=8 * seq * seq * width, bytes_accessed=8 * seq * width, transcendentals=0),
        name="attention",
    )(queries, keys, vals)


def dispatch_kernel(rank_ref, *refs, capacity):
    u_refs, x_ref = refs[:-1], refs[-1]
    local, n_tok = rank_ref.shape
    slots = lax.broadcasted_iota(jnp.int32, (capacity, n_tok), 0)
    picks = [(rank_ref[e:e + 1, :] == slots).astype(jnp.float32).astype(jnp.bfloat16) for e in range(local)]
    pick = jnp.concatenate(picks, axis=0)
    tokens = jnp.concatenate([u[...] for u in u_refs], axis=0)
    rows = jnp.dot(pick, tokens, preferred_element_type=jnp.float32).astype(jnp.bfloat16)
    for e in range(local):
        x_ref[e] = rows[e * capacity:(e + 1) * capacity, :]


def dispatch(rank, tokens, capacity):
    local, n_tok = rank.shape
    d_model = tokens[0].shape[1]
    width = 512
    return pl.pallas_call(
        functools.partial(dispatch_kernel, capacity=capacity),
        grid=(d_model // width,),
        in_specs=[pl.BlockSpec((local, n_tok), lambda c: (0, 0))] + [pl.BlockSpec((t.shape[0], width), lambda c: (0, c)) for t in tokens],
        out_specs=pl.BlockSpec((local, capacity, width), lambda c: (0, 0, c)),
        out_shape=jax.ShapeDtypeStruct((local, capacity, d_model), jnp.bfloat16),
        compiler_params=params(),
        cost_estimate=pl.CostEstimate(flops=2 * local * capacity * n_tok * d_model, bytes_accessed=4 * local * capacity * d_model, transcendentals=0),
        name="dispatch",
    )(rank, *tokens)


def expert_kernel(size_ref, start_ref, total_ref, *refs, n_src, chunk):
    x_refs, (gate_ref, up_ref, down_ref) = refs[:n_src], refs[n_src:n_src + 3]
    f_refs = refs[n_src + 3:2 * n_src + 3]
    x_buf, f_buf, in_sems, out_sems = refs[2 * n_src + 3:]
    e, local = pl.program_id(0), pl.num_programs(0)
    slot = lax.rem(e, 2)
    capacity, d_model = f_refs[0].shape[1:]
    zeros = jnp.zeros((capacity, d_model), jnp.bfloat16)

    def fetch(r, expert, where):
        size = pl.multiple_of(size_ref[r, expert], ALIGN)
        start = pl.multiple_of(start_ref[r, expert], ALIGN)
        return pltpu.make_async_copy(x_refs[r].at[expert, pl.ds(0, size), :], x_buf.at[where, pl.ds(start, size), :], in_sems.at[where, r])

    def put(r, expert, where):
        start = pl.multiple_of(start_ref[r, expert], ALIGN)
        return pltpu.make_async_copy(f_buf.at[where, pl.ds(start, capacity), :], f_refs[r].at[expert], out_sems.at[where, r])

    @pl.when(e == 0)
    def _():
        for r in range(n_src):
            fetch(r, 0, 0).start()

    @pl.when(e + 1 < local)
    def _():
        for r in range(n_src):
            fetch(r, e + 1, 1 - slot).start()

    for r in range(n_src):
        fetch(r, e, slot).wait()

    @pl.when(e >= 2)
    def _():
        for r in range(n_src):
            put(r, e - 2, slot).wait()

    total = total_ref[e]
    x_buf[slot, pl.ds(pl.multiple_of(total, ALIGN), capacity), :] = zeros
    chunks = (total + chunk - 1) // chunk

    @pl.loop(0, chunks)
    def _(i):
        rows = pl.ds(pl.multiple_of(i * chunk, chunk), chunk)
        x = x_buf[slot, rows, :]
        gate_act = jnp.dot(x, gate_ref[0], preferred_element_type=jnp.float32)
        up_act = jnp.dot(x, up_ref[0], preferred_element_type=jnp.float32)
        middle = (gate_act * jax.nn.sigmoid(gate_act) * up_act).astype(jnp.bfloat16)
        f_buf[slot, rows, :] = jnp.dot(middle, down_ref[0], preferred_element_type=jnp.float32).astype(jnp.bfloat16)

    f_buf[slot, pl.ds(pl.multiple_of(chunks * chunk, chunk), capacity), :] = zeros
    for r in range(n_src):
        put(r, e, slot).start()

    @pl.when(e == local - 1)
    def _():
        @pl.when(e >= 1)
        def _():
            for r in range(n_src):
                put(r, e - 1, 1 - slot).wait()
        for r in range(n_src):
            put(r, e, slot).wait()


def experts(sizes, starts, totals, rows, gate_w, up_w, down_w):
    n_src = len(rows)
    local, capacity, d_model = rows[0].shape
    width = gate_w.shape[2]
    chunk = capacity
    n_rows = n_src * capacity + 2 * capacity
    anywhere = pl.BlockSpec(memory_space=pl.ANY)
    return pl.pallas_call(
        functools.partial(expert_kernel, n_src=n_src, chunk=chunk),
        grid_spec=pltpu.PrefetchScalarGridSpec(
            num_scalar_prefetch=3,
            grid=(local,),
            in_specs=[anywhere] * n_src + [
                pl.BlockSpec((1, d_model, width), lambda e, *_: (e, 0, 0)),
                pl.BlockSpec((1, d_model, width), lambda e, *_: (e, 0, 0)),
                pl.BlockSpec((1, width, d_model), lambda e, *_: (e, 0, 0)),
            ],
            out_specs=[anywhere] * n_src,
            scratch_shapes=[
                pltpu.VMEM((2, n_rows, d_model), jnp.bfloat16),
                pltpu.VMEM((2, n_rows, d_model), jnp.bfloat16),
                pltpu.SemaphoreType.DMA((2, n_src)),
                pltpu.SemaphoreType.DMA((2, n_src)),
            ],
        ),
        out_shape=[jax.ShapeDtypeStruct(rows[0].shape, jnp.bfloat16)] * n_src,
        compiler_params=params(),
        cost_estimate=pl.CostEstimate(flops=4 * local * n_src * capacity * d_model * width, bytes_accessed=6 * local * d_model * width, transcendentals=0),
        name="experts",
    )(sizes, starts, totals, *rows, gate_w, up_w, down_w)


def combine_kernel(rank_ref, piece_ref, f_ref, *out_refs):
    n_tok, local = rank_ref.shape
    capacity = f_ref.shape[1]
    pieces = piece_ref.shape[1] // local
    slots = lax.broadcasted_iota(jnp.int32, (n_tok, capacity), 1)
    rank = rank_ref[...]
    weights = piece_ref[...]
    rows = [[] for _ in range(pieces)]
    for e in range(local):
        hit = rank[:, e:e + 1] == slots
        for k in range(pieces):
            column = k * local + e
            rows[k].append(jnp.where(hit, weights[:, column:column + 1], 0.0).astype(jnp.bfloat16))
    spread = [jnp.concatenate(r, axis=1) for r in rows]
    width = out_refs[0].shape[1]
    for c, out_ref in enumerate(out_refs):
        cols = slice(c * width, (c + 1) * width)
        data = jnp.concatenate([f_ref[e, :, cols] for e in range(local)], axis=0)
        total = jnp.dot(spread[0], data, preferred_element_type=jnp.float32)
        for k in range(1, pieces):
            total += jnp.dot(spread[k], data, preferred_element_type=jnp.float32)
        out_ref[...] = total


def combine(rank_t, pieces, results, half, outs):
    local, capacity, d_model = results.shape
    n_tok = rank_t.shape[0]
    width = d_model // 2
    whole = lambda i: (0, 0)
    return pl.pallas_call(
        combine_kernel,
        grid=(1,),
        in_specs=[
            pl.BlockSpec(rank_t.shape, whole),
            pl.BlockSpec(pieces.shape, whole),
            pl.BlockSpec((local, capacity, width), lambda i: (0, 0, half)),
        ],
        out_specs=[pl.BlockSpec((n_tok, width // outs), whole)] * outs,
        out_shape=[jax.ShapeDtypeStruct((n_tok, width // outs), jnp.float32)] * outs,
        compiler_params=params(),
        cost_estimate=pl.CostEstimate(flops=6 * local * capacity * n_tok * width, bytes_accessed=4 * local * capacity * width, transcendentals=0),
        name="combine",
    )(rank_t, pieces, results)


def project_kernel(order_ref, rows_ref, *refs):
    blocks, out_ref = refs[:-1], refs[-1]
    count = order_ref.shape[0]
    size = rows_ref.shape[1] // count
    rows = jnp.concatenate([rows_ref[:, pl.ds(pl.multiple_of(order_ref[j] * size, size), size)] for j in range(count)], axis=1)
    weight = jnp.concatenate([block[...] for block in blocks], axis=0)
    out_ref[...] = jnp.dot(rows, weight, preferred_element_type=jnp.float32).astype(out_ref.dtype)


def project(order, rows, blocks, dtype=jnp.bfloat16):
    n_rows, depth = rows.shape
    n_cols = blocks[0].shape[1]
    width = 512
    return pl.pallas_call(
        project_kernel,
        grid_spec=pltpu.PrefetchScalarGridSpec(
            num_scalar_prefetch=1,
            grid=(n_cols // width,),
            in_specs=[pl.BlockSpec((n_rows, depth), lambda c, *_: (0, 0))] + [pl.BlockSpec((b.shape[0], width), lambda c, *_: (0, c)) for b in blocks],
            out_specs=pl.BlockSpec((n_rows, width), lambda c, *_: (0, c)),
        ),
        out_shape=jax.ShapeDtypeStruct((n_rows, n_cols), dtype),
        compiler_params=params(),
        cost_estimate=pl.CostEstimate(flops=2 * n_rows * depth * n_cols, bytes_accessed=2 * depth * n_cols, transcendentals=0),
        name="project",
    )(order, rows, *blocks)


class Ring:
    def __init__(self, axis, group):
        self.axis = axis
        self.group = group
        me = lax.axis_index(axis)
        chip, core = me // 2, me % 2
        chips = [chip, chip - 1, chip + 1, chip + 2]
        self.order = jnp.stack([(c % (group // 2)) * 2 + side for side in (core, 1 - core) for c in chips]).astype(jnp.int32)

    def shift(self, values, chips):
        return lax.ppermute(values, self.axis, [(i, (i + 2 * chips) % self.group) for i in range(self.group)])

    def swap(self, values):
        return lax.ppermute(values, self.axis, [(i, i ^ 1) for i in range(self.group)])

    def gather(self, shard):
        half = shard.shape[0] // 2
        below, above = self.shift(shard, 1), self.shift(shard, -1)
        first, second = self.shift(below[:half], 1), self.shift(above[half:], -1)
        near = [(shard,), (below,), (above,), (first, second)]
        return near + [tuple(self.swap(part) for part in parts) for parts in near]

    def gather_small(self, values):
        near = jnp.stack([values, self.shift(values, 1), self.shift(values, -1), self.shift(values, 2)])
        return jnp.concatenate([near, self.swap(near)])


def flat(blocks):
    return [part for parts in blocks for part in parts]


def bf16_pieces(values):
    first = lax.reduce_precision(values, 8, 7)
    second = lax.reduce_precision(values - first, 8, 7)
    third = values - first - second
    return first, second, third


def local_layer(x_loc, q_shard, k_shard, v_shard, o_shard, w_router, gate_loc, up_loc, down_loc, sgate_shard, sup_shard, sdown_shard, ids_loc, group):
    n_seq, seq_len, d_model = x_loc.shape
    head = q_shard.shape[2]
    n_tok = n_seq * seq_len
    top_k = ids_loc.shape[-1]
    local = gate_loc.shape[0]
    n_experts = local * group
    capacity = CAP_FACTOR * n_tok * top_k // n_experts
    ring = Ring('ep', group)
    order = ring.order

    def gathered(shard):
        return flat(ring.gather(shard.reshape(shard.shape[0], -1)))

    ids_all = lax.all_gather(ids_loc.reshape(n_tok, top_k).T, 'ep', axis=0)[order]
    mine = lax.axis_index('ep') * local + jnp.arange(local)
    chosen = ids_all[:, None, :, :] == mine[None, :, None, None]
    member = jnp.any(chosen, axis=2)
    before = (jnp.arange(n_tok)[:, None] < jnp.arange(n_tok)[None, :]).astype(jnp.bfloat16)
    rank = jnp.einsum('set,tq->seq', member.astype(jnp.bfloat16), before, preferred_element_type=jnp.float32).astype(jnp.int32)
    rank = jnp.where(member, rank, -1)
    rank_t = rank.transpose(0, 2, 1)
    sizes = (jnp.sum(member.astype(jnp.int32), axis=2) + ALIGN - 1) // ALIGN * ALIGN
    ends = jnp.cumsum(sizes, axis=0)
    starts, totals = ends - sizes, ends[-1]

    x_flat = x_loc.reshape(n_tok, d_model)
    normed = rms_norm(x_flat).astype(jnp.bfloat16)
    keys_all = project(order, normed, gathered(k_shard))
    vals_all = project(order, normed, gathered(v_shard))
    queries = project(order, normed, gathered(q_shard))
    attended = [attention(queries[i * seq_len:(i + 1) * seq_len], keys_all[i * seq_len:(i + 1) * seq_len], vals_all[i * seq_len:(i + 1) * seq_len], head) for i in range(n_seq)]
    attended = attended[0] if n_seq == 1 else jnp.concatenate(attended, axis=0)
    attn_out = project(order, attended, gathered(o_shard))
    residual = (x_flat.astype(jnp.float32) + attn_out.astype(jnp.float32)).astype(jnp.bfloat16)

    hidden = rms_norm(residual)
    moe_in = hidden.astype(jnp.bfloat16)
    tokens = ring.gather(moe_in)
    logits = jnp.dot(hidden, w_router, precision=lax.Precision.HIGHEST, preferred_element_type=jnp.float32)
    tok_ids = ids_loc.reshape(n_tok, top_k)
    picked = tok_ids[:, :, None] == jnp.arange(n_experts)[None, None, :]
    chosen_logits = jnp.sum(jnp.where(picked, logits[:, None, :], 0.0), axis=2)
    gate_probs = jax.nn.softmax(chosen_logits, axis=-1)
    gates_all = ring.gather_small(gate_probs.T)
    weight = jnp.sum(jnp.where(chosen, gates_all[:, None, :, :], 0.0), axis=2)
    pieces = jnp.concatenate(bf16_pieces(weight), axis=1).transpose(0, 2, 1)

    rows = [dispatch(rank[r], tokens[r], capacity) for r in range(group)]
    results = experts(sizes, starts, totals, rows, gate_loc, up_loc, down_loc)

    gate_act = project(order, moe_in, gathered(sgate_shard), jnp.float32)
    up_act = project(order, moe_in, gathered(sup_shard), jnp.float32)
    middle = (jax.nn.silu(gate_act) * up_act).astype(jnp.bfloat16)
    shared = project(order, middle, gathered(sdown_shard))

    chips = group // 2
    parts = 2
    routed = []
    for half, step, targets in ((0, 1, (1, 3, 2, 0)), (1, -1, (2, 3, 1, 0))):
        moving = None
        for target in targets:
            other = combine(rank_t[chips + target], pieces[chips + target], results[chips + target], half, parts)
            own = combine(rank_t[target], pieces[target], results[target], half, parts)
            totals_now = [a + ring.swap(b) for a, b in zip(own, other)]
            if moving is not None:
                totals_now = [a + b for a, b in zip(totals_now, moving)]
            moving = [ring.shift(t, step) for t in totals_now] if target else None
        routed += totals_now
    routed = jnp.concatenate(routed, axis=1)
    y_out = (residual.astype(jnp.float32) + routed + shared.astype(jnp.float32)).astype(jnp.bfloat16)
    return y_out.reshape(n_seq, seq_len, d_model)


def solution(mesh):
    tok_spec = P(('dp', 'ep'), None, None)
    row_spec = P('ep', None)
    cube_spec = P('ep', None, None)
    in_specs = (tok_spec, cube_spec, cube_spec, cube_spec, row_spec, P(None, None), cube_spec, cube_spec, cube_spec, row_spec, row_spec, row_spec, tok_spec)
    return jax.shard_map(functools.partial(local_layer, group=mesh.shape['ep']), mesh=mesh, in_specs=in_specs, out_specs=tok_spec, check_vma=False)
```

```python
import functools
import jax
import jax.numpy as jnp
from jax import lax
from jax.experimental import pallas as pl
from jax.experimental.pallas import tpu as pltpu
from jax.sharding import PartitionSpec as P

EPSILON = 1e-6
CAP_FACTOR = 2
ALIGN = 16
VMEM_BYTES = 60 * 1024 * 1024
MAX_VMEM = 67043328


def rms_norm(values):
    as_f32 = values.astype(jnp.float32)
    return as_f32 * lax.rsqrt(jnp.mean(as_f32 * as_f32, axis=-1, keepdims=True) + EPSILON)


def params(**kw):
    return pltpu.CompilerParams(vmem_limit_bytes=VMEM_BYTES, **kw)


def attention_kernel(q_ref, k_ref, v_ref, o_ref, *, parts):
    seq, head = q_ref.shape
    step = seq // parts
    for part in range(parts):
        lo, hi = part * step, (part + 1) * step
        scores = lax.dot_general(q_ref[lo:hi, :], k_ref[:hi, :], (((1,), (1,)), ((), ())), preferred_element_type=jnp.float32) * (head ** -0.5)
        rows = lo + lax.broadcasted_iota(jnp.int32, scores.shape, 0)
        cols = lax.broadcasted_iota(jnp.int32, scores.shape, 1)
        scores = jnp.where(rows >= cols, scores, -1e30)
        weights = jnp.exp(scores - jnp.max(scores, axis=-1, keepdims=True))
        probs = (weights / jnp.sum(weights, axis=-1, keepdims=True)).astype(jnp.bfloat16)
        o_ref[lo:hi, :] = jnp.dot(probs, v_ref[:hi, :], preferred_element_type=jnp.float32).astype(jnp.bfloat16)


def attention(queries, keys, vals, head):
    seq, width = queries.shape
    spec = pl.BlockSpec((seq, head), lambda i: (0, i))
    return pl.pallas_call(
        functools.partial(attention_kernel, parts=2),
        grid=(width // head,),
        in_specs=[spec] * 3,
        out_specs=spec,
        out_shape=jax.ShapeDtypeStruct((seq, width), jnp.bfloat16),
        compiler_params=params(),
        cost_estimate=pl.CostEstimate(flops=8 * seq * seq * width, bytes_accessed=8 * seq * width, transcendentals=0),
        name="attention",
    )(queries, keys, vals)


def dispatch_kernel(order_ref, rank_ref, u_ref, x_ref, *, capacity):
    local, n_tok = rank_ref.shape[1:]
    slots = lax.broadcasted_iota(jnp.int32, (capacity, n_tok), 0)
    picks = [(rank_ref[0, e:e + 1, :] == slots).astype(jnp.float32).astype(jnp.bfloat16) for e in range(local)]
    pick = jnp.concatenate(picks, axis=0)
    width = 512
    for c in range(u_ref.shape[2] // width):
        cols = slice(c * width, (c + 1) * width)
        rows = jnp.dot(pick, u_ref[0, :, cols], preferred_element_type=jnp.float32).astype(jnp.bfloat16)
        for e in range(local):
            x_ref[0, e, :, cols] = rows[e * capacity:(e + 1) * capacity, :]


def dispatch(order, rank, tokens, capacity):
    n_src, local, n_tok = rank.shape
    d_model = tokens.shape[2]
    return pl.pallas_call(
        functools.partial(dispatch_kernel, capacity=capacity),
        grid_spec=pltpu.PrefetchScalarGridSpec(
            num_scalar_prefetch=1,
            grid=(n_src,),
            in_specs=[pl.BlockSpec((1, local, n_tok), lambda s, order: (s, 0, 0)), pl.BlockSpec((1, n_tok, d_model), lambda s, order: (order[s], 0, 0))],
            out_specs=pl.BlockSpec((1, local, capacity, d_model), lambda s, order: (s, 0, 0, 0)),
        ),
        out_shape=jax.ShapeDtypeStruct((n_src, local, capacity, d_model), jnp.bfloat16),
        compiler_params=params(),
        cost_estimate=pl.CostEstimate(flops=2 * n_src * local * capacity * n_tok * d_model, bytes_accessed=4 * n_src * local * capacity * d_model, transcendentals=0),
        name="dispatch",
    )(order, rank, tokens)


def expert_kernel(size_ref, start_ref, total_ref, x_ref, gate_ref, up_ref, down_ref, f_ref, x_buf, f_buf, in_sems, out_sems, *, chunk):
    n_src, _, capacity, d_model = x_ref.shape
    e, local = pl.program_id(0), pl.num_programs(0)
    slot = lax.rem(e, 2)
    zeros = jnp.zeros((capacity, d_model), jnp.bfloat16)

    def fetch(r, expert, where):
        size = pl.multiple_of(size_ref[r, expert], ALIGN)
        start = pl.multiple_of(start_ref[r, expert], ALIGN)
        return pltpu.make_async_copy(x_ref.at[r, expert, pl.ds(0, size), :], x_buf.at[where, pl.ds(start, size), :], in_sems.at[where, r])

    def put(r, expert, where):
        start = pl.multiple_of(start_ref[r, expert], ALIGN)
        return pltpu.make_async_copy(f_buf.at[where, pl.ds(start, capacity), :], f_ref.at[r, expert], out_sems.at[where, r])

    @pl.when(e == 0)
    def _():
        for r in range(n_src):
            fetch(r, 0, 0).start()

    @pl.when(e + 1 < local)
    def _():
        for r in range(n_src):
            fetch(r, e + 1, 1 - slot).start()

    for r in range(n_src):
        fetch(r, e, slot).wait()

    @pl.when(e >= 2)
    def _():
        for r in range(n_src):
            put(r, e - 2, slot).wait()

    total = total_ref[e]
    x_buf[slot, pl.ds(pl.multiple_of(total, ALIGN), capacity), :] = zeros
    chunks = (total + chunk - 1) // chunk

    @pl.loop(0, chunks)
    def _(i):
        rows = pl.ds(pl.multiple_of(i * chunk, chunk), chunk)
        x = x_buf[slot, rows, :]
        gate_act = jnp.dot(x, gate_ref[0], preferred_element_type=jnp.float32)
        up_act = jnp.dot(x, up_ref[0], preferred_element_type=jnp.float32)
        middle = (gate_act * jax.nn.sigmoid(gate_act) * up_act).astype(jnp.bfloat16)
        f_buf[slot, rows, :] = jnp.dot(middle, down_ref[0], preferred_element_type=jnp.float32).astype(jnp.bfloat16)

    f_buf[slot, pl.ds(pl.multiple_of(chunks * chunk, chunk), capacity), :] = zeros
    for r in range(n_src):
        put(r, e, slot).start()

    @pl.when(e == local - 1)
    def _():
        @pl.when(e >= 1)
        def _():
            for r in range(n_src):
                put(r, e - 1, 1 - slot).wait()
        for r in range(n_src):
            put(r, e, slot).wait()


def experts(sizes, starts, totals, rows, gate_w, up_w, down_w):
    n_src, local, capacity, d_model = rows.shape
    width = gate_w.shape[2]
    chunk = capacity
    n_rows = n_src * capacity + 2 * capacity
    anywhere = pl.BlockSpec(memory_space=pl.ANY)
    return pl.pallas_call(
        functools.partial(expert_kernel, chunk=chunk),
        grid_spec=pltpu.PrefetchScalarGridSpec(
            num_scalar_prefetch=3,
            grid=(local,),
            in_specs=[anywhere] + [
                pl.BlockSpec((1, d_model, width), lambda e, *_: (e, 0, 0)),
                pl.BlockSpec((1, d_model, width), lambda e, *_: (e, 0, 0)),
                pl.BlockSpec((1, width, d_model), lambda e, *_: (e, 0, 0)),
            ],
            out_specs=anywhere,
            scratch_shapes=[
                pltpu.VMEM((2, n_rows, d_model), jnp.bfloat16),
                pltpu.VMEM((2, n_rows, d_model), jnp.bfloat16),
                pltpu.SemaphoreType.DMA((2, n_src)),
                pltpu.SemaphoreType.DMA((2, n_src)),
            ],
        ),
        out_shape=jax.ShapeDtypeStruct(rows.shape, jnp.bfloat16),
        compiler_params=params(),
        cost_estimate=pl.CostEstimate(flops=4 * local * n_src * capacity * d_model * width, bytes_accessed=6 * local * d_model * width, transcendentals=0),
        name="experts",
    )(sizes, starts, totals, rows, gate_w, up_w, down_w)


def neighbour(chips, swap=False):
    me, group = lax.axis_index('ep'), lax.axis_size('ep')
    side = lax.rem(me, 2)
    chip = lax.rem(me // 2 + chips + group // 2, group // 2)
    return {'ep': chip * 2 + (1 - side if swap else side)}


def greet():
    barrier = pltpu.get_barrier_semaphore()
    for device in (neighbour(1), neighbour(-1), neighbour(0, True)):
        pl.semaphore_signal(barrier, inc=1, device_id=device, device_id_type=pl.DeviceIdType.MESH)
    pl.semaphore_wait(barrier, 3)


def remote(src, dst, send_sem, recv_sem, device):
    return pltpu.make_async_remote_copy(src_ref=src, dst_ref=dst, send_sem=send_sem, recv_sem=recv_sem, device_id=device, device_id_type=pl.DeviceIdType.MESH)


def reduce_kernel(rank_ref, piece_ref, f_ref, out_ref, f_buf, spread, other_buf, swap_buf, send_buf, ring_buf, f_sems, swap_send, swap_recv, ring_send, ring_recv, out_sems, free_sem):
    n_src, n_tok, local = rank_ref.shape
    capacity = f_ref.shape[2]
    pieces = piece_ref.shape[2] // local
    chips = n_src // 2
    width = out_ref.shape[1] // 4
    n_units = 16

    def quarter(u):
        return 2 * lax.rem(u, 2) + u // 2

    def place(i):
        u = lax.rem(i, 4)
        odd = lax.rem(u, 2)
        target = jnp.where(i < 4, 1 + odd, jnp.where(i < 8, 2 - odd, jnp.where(i < 12, 3, 0)))
        return u, target

    def fetch(i, side, slot):
        u, target = place(i)
        cols = pl.ds(pl.multiple_of(quarter(u) * width, width), width)
        return pltpu.make_async_copy(f_ref.at[target + chips * (1 - side), :, :, cols], f_buf.at[slot, side], f_sems.at[slot, side])

    def swap_copy(i):
        s = lax.rem(i, 4)
        return remote(other_buf.at[s], swap_buf.at[s], swap_send.at[s], swap_recv.at[s], neighbour(0, True))

    def ring_copy(source, slot):
        return remote(send_buf.at[source], ring_buf.at[slot], ring_send.at[slot], ring_recv.at[slot], neighbour(1 - 2 * lax.rem(slot, 2)))

    def build(target, entry):
        @pl.loop(0, 2)
        def _(side):
            r = target + chips * (1 - side)
            rank = rank_ref[r]
            weights = piece_ref[r]
            slots = lax.broadcasted_iota(jnp.int32, (n_tok, capacity), 1)
            for e in range(local):
                hit = rank[:, e:e + 1] == slots
                for k in range(pieces):
                    column = k * local + e
                    spread[entry * 2 + side, k, :, e * capacity:(e + 1) * capacity] = jnp.where(hit, weights[:, column:column + 1], 0.0).astype(jnp.bfloat16)

    def product(entry, slot, side):
        data = jnp.concatenate([f_buf[slot, side, e] for e in range(local)], axis=0)
        total = jnp.dot(spread[entry * 2 + side, 0], data, preferred_element_type=jnp.float32)
        for k in range(1, pieces):
            total += jnp.dot(spread[entry * 2 + side, k], data, preferred_element_type=jnp.float32)
        return total

    for side in range(2):
        fetch(0, side, 0).start()
    greet()

    @pl.loop(0, n_units)
    def _(i):
        u, target = place(i)
        slot = lax.rem(i, 2)
        lane = lax.rem(i, 4)

        @pl.when(i + 1 < n_units)
        def _():
            for side in range(2):
                fetch(i + 1, side, 1 - slot).start()

        @pl.when(i == 0)
        def _():
            build(1, 0)

        @pl.when(i == 1)
        def _():
            build(2, 1)

        @pl.when(i == 8)
        def _():
            build(3, 0)

        @pl.when(i == 12)
        def _():
            build(0, 1)

        entry = 1 - lax.rem(target, 2)

        @pl.when(i >= 4)
        def _():
            swap_copy(i - 4).wait_send()
            pl.semaphore_wait(free_sem, 1)

        fetch(i, 0, slot).wait()
        other_buf[lane] = product(entry, slot, 0)
        swap_copy(i).start()
        fetch(i, 1, slot).wait()
        send_buf[i] = product(entry, slot, 1)
        swap_copy(i).wait_recv()
        send_buf[i] += swap_buf[lane]

        @pl.when(i < n_units - 4)
        def _():
            pl.semaphore_signal(free_sem, inc=1, device_id=neighbour(0, True), device_id_type=pl.DeviceIdType.MESH)

        @pl.when(i < 4)
        def _():
            ring_copy(i, u).start()

        @pl.when((i >= 8) & (i < 12))
        def _():
            ring_copy(i, u).wait_recv()
            send_buf[i] += ring_buf[u]
            ring_copy(i, u + 4).start()

    @pl.loop(0, 4)
    def _(u):
        ring_copy(0, u + 4).wait_recv()
        send_buf[u + 4] += ring_buf[u + 4]
        ring_copy(u + 4, u + 8).start()

    def put(u):
        cols = pl.ds(pl.multiple_of(quarter(u) * width, width), width)
        return pltpu.make_async_copy(send_buf.at[12 + u], out_ref.at[:, cols], out_sems.at[u])

    @pl.loop(0, 4)
    def _(u):
        ring_copy(0, u + 8).wait_recv()
        send_buf[12 + u] += ring_buf[u + 8]
        put(u).start()

    @pl.loop(0, 4)
    def _(u):
        put(u).wait()
        swap_copy(n_units - 4 + u).wait_send()
        ring_copy(u, u).wait_send()
        ring_copy(8 + u, u + 4).wait_send()
        ring_copy(4 + u, u + 8).wait_send()


def reduce_results(rank_t, pieces, results):
    n_src, local, capacity, d_model = results.shape
    n_tok = rank_t.shape[1]
    width = d_model // 4
    n_pieces = pieces.shape[2] // local
    tile = (n_tok, width)
    vmem = pl.BlockSpec(memory_space=pltpu.VMEM)
    return pl.pallas_call(
        reduce_kernel,
        in_specs=[vmem, vmem, pl.BlockSpec(memory_space=pl.ANY)],
        out_specs=pl.BlockSpec(memory_space=pl.ANY),
        out_shape=jax.ShapeDtypeStruct((n_tok, d_model), jnp.float32),
        scratch_shapes=[
            pltpu.VMEM((2, 2, local, capacity, width), jnp.bfloat16),
            pltpu.VMEM((4, n_pieces, n_tok, local * capacity), jnp.bfloat16),
            pltpu.VMEM((4,) + tile, jnp.float32),
            pltpu.VMEM((4,) + tile, jnp.float32),
            pltpu.VMEM((16,) + tile, jnp.float32),
            pltpu.VMEM((12,) + tile, jnp.float32),
            pltpu.SemaphoreType.DMA((2, 2)),
            pltpu.SemaphoreType.DMA((4,)),
            pltpu.SemaphoreType.DMA((4,)),
            pltpu.SemaphoreType.DMA((12,)),
            pltpu.SemaphoreType.DMA((12,)),
            pltpu.SemaphoreType.DMA((4,)),
            pltpu.SemaphoreType.REGULAR,
        ],
        compiler_params=pltpu.CompilerParams(vmem_limit_bytes=MAX_VMEM, collective_id=2, has_side_effects=True),
        cost_estimate=pl.CostEstimate(flops=6 * n_src * local * capacity * n_tok * d_model, bytes_accessed=4 * n_src * local * capacity * d_model, transcendentals=0),
        name="reduce_results",
    )(rank_t, pieces, results)


def bf16_pieces(values):
    first = lax.reduce_precision(values, 8, 7)
    second = lax.reduce_precision(values - first, 8, 7)
    third = values - first - second
    return first, second, third


def local_layer(x_loc, q_shard, k_shard, v_shard, o_shard, w_router, gate_loc, up_loc, down_loc, sgate_shard, sup_shard, sdown_shard, ids_loc, group):
    n_seq, seq_len, d_model = x_loc.shape
    head = q_shard.shape[2]
    n_tok = n_seq * seq_len
    top_k = ids_loc.shape[-1]
    local = gate_loc.shape[0]
    n_experts = local * group
    capacity = CAP_FACTOR * n_tok * top_k // n_experts
    me = lax.axis_index('ep')
    chips = [me // 2 + step for step in (0, -1, 1, 2)]
    order = jnp.stack([(c % (group // 2)) * 2 + side for side in (me % 2, 1 - me % 2) for c in chips]).astype(jnp.int32)

    def gathered(shard):
        return lax.all_gather(shard.reshape(shard.shape[0], -1), 'ep', axis=0, tiled=True)

    def project(rows, weight):
        return jnp.dot(rows, weight, preferred_element_type=jnp.float32).astype(jnp.bfloat16)

    ids_all = lax.all_gather(ids_loc.reshape(n_tok, top_k).T, 'ep', axis=0)[order]
    mine = lax.axis_index('ep') * local + jnp.arange(local)
    chosen = ids_all[:, None, :, :] == mine[None, :, None, None]
    member = jnp.any(chosen, axis=2)
    before = (jnp.arange(n_tok)[:, None] < jnp.arange(n_tok)[None, :]).astype(jnp.bfloat16)
    rank = jnp.einsum('set,tq->seq', member.astype(jnp.bfloat16), before, preferred_element_type=jnp.float32).astype(jnp.int32)
    rank = jnp.where(member, rank, -1)
    rank_t = rank.transpose(0, 2, 1)
    sizes = (jnp.sum(member.astype(jnp.int32), axis=2) + ALIGN - 1) // ALIGN * ALIGN
    ends = jnp.cumsum(sizes, axis=0)
    starts, totals = ends - sizes, ends[-1]

    x_flat = x_loc.reshape(n_tok, d_model)
    normed = rms_norm(x_flat).astype(jnp.bfloat16)
    keys_all = project(normed, gathered(k_shard))
    vals_all = project(normed, gathered(v_shard))
    queries = project(normed, gathered(q_shard))
    attended = [attention(queries[i * seq_len:(i + 1) * seq_len], keys_all[i * seq_len:(i + 1) * seq_len], vals_all[i * seq_len:(i + 1) * seq_len], head) for i in range(n_seq)]
    attended = attended[0] if n_seq == 1 else jnp.concatenate(attended, axis=0)
    attn_out = project(attended, gathered(o_shard))
    residual = (x_flat.astype(jnp.float32) + attn_out.astype(jnp.float32)).astype(jnp.bfloat16)

    hidden = rms_norm(residual)
    moe_in = hidden.astype(jnp.bfloat16)
    tokens = lax.all_gather(moe_in, 'ep', axis=0)
    logits = jnp.dot(hidden, w_router, precision=lax.Precision.HIGHEST, preferred_element_type=jnp.float32)
    tok_ids = ids_loc.reshape(n_tok, top_k)
    picked = tok_ids[:, :, None] == jnp.arange(n_experts)[None, None, :]
    chosen_logits = jnp.sum(jnp.where(picked, logits[:, None, :], 0.0), axis=2)
    gate_probs = jax.nn.softmax(chosen_logits, axis=-1)
    gates_all = lax.all_gather(gate_probs.T, 'ep', axis=0)[order]
    weight = jnp.sum(jnp.where(chosen, gates_all[:, None, :, :], 0.0), axis=2)
    pieces = jnp.concatenate(bf16_pieces(weight), axis=1).transpose(0, 2, 1)

    rows = dispatch(order, rank, tokens, capacity)
    results = experts(sizes, starts, totals, rows, gate_loc, up_loc, down_loc)

    gate_act = jnp.dot(moe_in, gathered(sgate_shard), preferred_element_type=jnp.float32)
    up_act = jnp.dot(moe_in, gathered(sup_shard), preferred_element_type=jnp.float32)
    middle = (jax.nn.silu(gate_act) * up_act).astype(jnp.bfloat16)
    shared = project(middle, gathered(sdown_shard))
    routed = reduce_results(rank_t, pieces, results)
    y_out = (residual.astype(jnp.float32) + routed + shared.astype(jnp.float32)).astype(jnp.bfloat16)
    return y_out.reshape(n_seq, seq_len, d_model)


def solution(mesh):
    tok_spec = P(('dp', 'ep'), None, None)
    row_spec = P('ep', None)
    cube_spec = P('ep', None, None)
    in_specs = (tok_spec, cube_spec, cube_spec, cube_spec, row_spec, P(None, None), cube_spec, cube_spec, cube_spec, row_spec, row_spec, row_spec, tok_spec)
    return jax.shard_map(functools.partial(local_layer, group=mesh.shape['ep']), mesh=mesh, in_specs=in_specs, out_specs=tok_spec, check_vma=False)
```

```python
import functools
import jax
import jax.numpy as jnp
from jax import lax
from jax.experimental import pallas as pl
from jax.experimental.pallas import tpu as pltpu
from jax.sharding import PartitionSpec as P

EPSILON = 1e-6
CAP_FACTOR = 2
ALIGN = 16
VMEM_BYTES = 60 * 1024 * 1024
MAX_VMEM = 67043328


def rms_norm(values):
    as_f32 = values.astype(jnp.float32)
    return as_f32 * lax.rsqrt(jnp.mean(as_f32 * as_f32, axis=-1, keepdims=True) + EPSILON)


def params(**kw):
    return pltpu.CompilerParams(vmem_limit_bytes=VMEM_BYTES, **kw)


def neighbour(chips, swap=False):
    me, group = lax.axis_index('ep'), lax.axis_size('ep')
    side = lax.rem(me, 2)
    chip = lax.rem(me // 2 + chips + group // 2, group // 2)
    return {'ep': chip * 2 + (1 - side if swap else side)}


def greet(*devices):
    barrier = pltpu.get_barrier_semaphore()
    for device in devices:
        pl.semaphore_signal(barrier, inc=1, device_id=device, device_id_type=pl.DeviceIdType.MESH)
    pl.semaphore_wait(barrier, len(devices))


def remote(src, dst, send_sem, recv_sem, device):
    return pltpu.make_async_remote_copy(src_ref=src, dst_ref=dst, send_sem=send_sem, recv_sem=recv_sem, device_id=device, device_id_type=pl.DeviceIdType.MESH)


class Gather:
    def __init__(self, buf, send, recv, split=True):
        other = neighbour(0, True)
        half = buf.shape[1] // 2
        lo, hi = pl.ds(0, half), pl.ds(half, half)

        def copy(k, src, dst, device):
            return remote(src, dst, send.at[k], recv.at[k], device)

        self.own = [copy(0, buf.at[0], buf.at[1], neighbour(1)), copy(1, buf.at[0], buf.at[2], neighbour(-1))]
        self.mate = [copy(2, buf.at[0], buf.at[4], other)]
        self.near_mate = [copy(3, buf.at[1], buf.at[5], other), copy(4, buf.at[2], buf.at[6], other)]
        if split:
            self.far = [copy(5, buf.at[1, lo], buf.at[3, lo], neighbour(1)), copy(6, buf.at[2, hi], buf.at[3, hi], neighbour(-1))]
            self.far_mate = [copy(7, buf.at[3, lo], buf.at[7, lo], other), copy(8, buf.at[3, hi], buf.at[7, hi], other)]
        else:
            self.far = [copy(5, buf.at[0], buf.at[3], neighbour(2))]
            self.far_mate = [copy(7, buf.at[3], buf.at[7], other)]
        self.split = split

    def begin(self):
        for copy in self.own + self.mate + ([] if self.split else self.far):
            copy.start()

    def forward(self):
        for k in range(2):
            self.own[k].wait_recv()
            if self.split:
                self.far[k].start()
            self.near_mate[k].start()

    def forward_far(self):
        for copy, mate in zip(self.far, self.far_mate):
            copy.wait_recv()
            mate.start()

    def arrive(self, copies):
        for copy in copies:
            copy.wait_recv()

    def finish(self):
        for copy in self.own + self.mate + self.near_mate + self.far + self.far_mate:
            copy.wait_send()


def owner(r):
    step = (0, -1, 1, 2)[r % 4]
    return neighbour(step, r >= 4)['ep']


def attention_layer_kernel(x_ref, ids_ref, k_hbm, v_hbm, q_hbm, o_hbm, h_ref, rank_ref, ids_out, w_buf, n_buf, qkv, ids_buf, load_sems, send, recv, ids_send, ids_recv):
    n_tok, d_model = x_ref.shape
    group, local = rank_ref.shape[:2]
    size = d_model // group
    head = 128
    width = 512
    keys, vals, queries, outs = range(4)
    gathers = [Gather(w_buf.at[w], send.at[w], recv.at[w]) for w in range(4)]
    ids_gather = Gather(ids_buf, ids_send, ids_recv, split=False)
    loads = [pltpu.make_async_copy(ref, w_buf.at[w, 0], load_sems.at[w]) for w, ref in enumerate((k_hbm, v_hbm, q_hbm, o_hbm))]
    ids_load = pltpu.make_async_copy(ids_ref, ids_buf.at[0], load_sems.at[4])
    ids_load.start()
    for load in loads:
        load.start()
    greet(neighbour(1), neighbour(-1), neighbour(2), neighbour(0, True))
    ids_load.wait()
    ids_gather.begin()
    for w in (keys, vals):
        loads[w].wait()
        gathers[w].begin()

    @pl.loop(0, n_tok // 128)
    def _(i):
        rows = pl.ds(pl.multiple_of(i * 128, 128), 128)
        normed = rms_norm(x_ref[rows, :]).astype(jnp.bfloat16)
        qkv[0, rows, :] = normed
        for r in range(group):
            n_buf[rows, r * size:(r + 1) * size] = qkv[0, rows, pl.ds(pl.multiple_of(owner(r) * size, size), size)]

    ids_gather.arrive(ids_gather.own + ids_gather.mate)
    for copy in ids_gather.near_mate:
        copy.start()
    ids_gather.forward_far()
    ids_gather.arrive(ids_gather.near_mate + ids_gather.far_mate)
    first = lax.axis_index('ep') * local
    before = (lax.broadcasted_iota(jnp.int32, (n_tok, n_tok), 0) < lax.broadcasted_iota(jnp.int32, (n_tok, n_tok), 1)).astype(jnp.float32).astype(jnp.bfloat16)
    for r in range(group):
        member = jnp.concatenate([jnp.max((ids_buf[r] == first + e).astype(jnp.float32), axis=0, keepdims=True) for e in range(local)], axis=0)
        rank = jnp.dot(member.astype(jnp.bfloat16), before, preferred_element_type=jnp.float32)
        rank_ref[r] = jnp.where(member > 0.5, rank, -1.0).astype(jnp.int32)

    def project(w, store):
        @pl.loop(0, d_model // width)
        def _(c):
            cols = pl.ds(pl.multiple_of(c * width, width), width)
            weight = jnp.concatenate([w_buf[w, r, :, cols] for r in range(group)], axis=0)
            store(cols, jnp.dot(n_buf[...], weight, preferred_element_type=jnp.float32).astype(jnp.bfloat16))

    def keep(w):
        def store(cols, values):
            qkv[w, :, cols] = values
        return store

    def complete(w):
        gathers[w].forward_far()
        gathers[w].arrive(gathers[w].mate + gathers[w].near_mate + gathers[w].far_mate)

    def attend(lo, hi):
        for r in range(lo, hi):
            start = owner(r) * size

            @pl.loop(0, size // head)
            def _(k):
                cols = pl.ds(pl.multiple_of(start + k * head, head), head)
                parts = 2
                step = n_tok // parts
                for part in range(parts):
                    top, end = part * step, (part + 1) * step
                    scores = lax.dot_general(qkv[queries, top:end, cols], qkv[keys, :end, cols], (((1,), (1,)), ((), ())), preferred_element_type=jnp.float32) * (head ** -0.5)
                    row = top + lax.broadcasted_iota(jnp.int32, scores.shape, 0)
                    col = lax.broadcasted_iota(jnp.int32, scores.shape, 1)
                    scores = jnp.where(row >= col, scores, -1e30)
                    weights = jnp.exp(scores - jnp.max(scores, axis=-1, keepdims=True))
                    probs = (weights / jnp.sum(weights, axis=-1, keepdims=True)).astype(jnp.bfloat16)
                    n_buf[top:end, pl.ds(pl.multiple_of(r * size + k * head, head), head)] = jnp.dot(probs, qkv[vals, :end, cols], preferred_element_type=jnp.float32).astype(jnp.bfloat16)

    gathers[keys].forward()
    loads[queries].wait()
    gathers[queries].begin()
    gathers[vals].forward()
    complete(keys)
    project(keys, keep(keys))
    gathers[queries].forward()
    loads[outs].wait()
    gathers[outs].begin()
    complete(vals)
    project(vals, keep(vals))
    complete(queries)
    project(queries, keep(queries))
    attend(0, group // 2)
    gathers[outs].forward()
    attend(group // 2, group)
    complete(outs)

    def residual(cols, values):
        h_ref[:, cols] = (x_ref[:, cols].astype(jnp.float32) + values.astype(jnp.float32)).astype(jnp.bfloat16)

    project(outs, residual)
    for r in range(group):
        ids_out[r] = ids_buf[r]
    for gather in gathers + [ids_gather]:
        gather.finish()


def attention_layer(x, ids_t, k_shard, v_shard, q_shard, o_shard, group, local):
    n_tok, d_model = x.shape
    top_k = ids_t.shape[0]
    vmem = pl.BlockSpec(memory_space=pltpu.VMEM)
    anywhere = pl.BlockSpec(memory_space=pl.ANY)
    return pl.pallas_call(
        attention_layer_kernel,
        in_specs=[vmem] + [anywhere] * 5,
        out_specs=[vmem] * 3,
        out_shape=[jax.ShapeDtypeStruct(x.shape, jnp.bfloat16), jax.ShapeDtypeStruct((group, local, n_tok), jnp.int32), jax.ShapeDtypeStruct((group, top_k, n_tok), jnp.int32)],
        scratch_shapes=[
            pltpu.VMEM((4, group) + k_shard.shape, jnp.bfloat16),
            pltpu.VMEM(x.shape, jnp.bfloat16),
            pltpu.VMEM((3,) + x.shape, jnp.bfloat16),
            pltpu.VMEM((group, top_k, n_tok), jnp.int32),
            pltpu.SemaphoreType.DMA((5,)),
            pltpu.SemaphoreType.DMA((4, 9)),
            pltpu.SemaphoreType.DMA((4, 9)),
            pltpu.SemaphoreType.DMA((9,)),
            pltpu.SemaphoreType.DMA((9,)),
        ],
        compiler_params=pltpu.CompilerParams(vmem_limit_bytes=MAX_VMEM, collective_id=0, has_side_effects=True),
        cost_estimate=pl.CostEstimate(flops=9 * n_tok * d_model * d_model, bytes_accessed=8 * d_model * d_model // group, transcendentals=0),
        name="attention_layer",
    )(x, ids_t, k_shard, v_shard, q_shard, o_shard)


def dispatch_kernel(h_ref, wr_ref, ids_ref, rank_ref, x_hbm, gates_ref, u_buf, pick, stage, g_buf, out_sems, send, recv, g_send, g_recv):
    n_tok, d_model = h_ref.shape
    group, local = rank_ref.shape[:2]
    capacity = x_hbm.shape[2]
    n_experts = wr_ref.shape[0]
    top_k = ids_ref.shape[0]
    width = stage.shape[3]
    n_cols = d_model // width
    tokens = Gather(u_buf, send, recv)
    gates = Gather(g_buf, g_send, g_recv, split=False)

    @pl.loop(0, n_tok // 128)
    def _(i):
        rows = pl.ds(pl.multiple_of(i * 128, 128), 128)
        u_buf[0, rows, :] = rms_norm(h_ref[rows, :]).astype(jnp.bfloat16)

    greet(neighbour(1), neighbour(-1), neighbour(2), neighbour(0, True))
    tokens.begin()

    for i in range(n_tok // 128):
        rows = slice(i * 128, (i + 1) * 128)
        logits = lax.dot_general(wr_ref[...], rms_norm(h_ref[rows, :]), (((1,), (1,)), ((), ())), precision=lax.Precision.HIGHEST, preferred_element_type=jnp.float32)
        experts_iota = lax.broadcasted_iota(jnp.int32, (n_experts, 128), 0)
        chosen = jnp.concatenate([jnp.sum(jnp.where(experts_iota == ids_ref[j:j + 1, rows], logits, 0.0), axis=0, keepdims=True) for j in range(top_k)], axis=0)
        weights = jnp.exp(chosen - jnp.max(chosen, axis=0, keepdims=True))
        g_buf[0, :, rows] = weights / jnp.sum(weights, axis=0, keepdims=True)
    gates.begin()

    def put(r, c, slot):
        cols = pl.ds(pl.multiple_of(c * width, width), width)
        return pltpu.make_async_copy(stage.at[slot], x_hbm.at[r, :, :, cols], out_sems.at[slot])

    def dispatch(r, before):
        slots = lax.broadcasted_iota(jnp.int32, (capacity, n_tok), 0)
        for e in range(local):
            pick[e * capacity:(e + 1) * capacity, :] = (rank_ref[r, e:e + 1, :] == slots).astype(jnp.float32).astype(jnp.bfloat16)

        @pl.loop(0, n_cols)
        def _(c):
            slot = lax.rem(c, 2)
            cols = pl.ds(pl.multiple_of(c * width, width), width)
            if before is None:
                @pl.when(c >= 2)
                def _():
                    put(r, c - 2, slot).wait()
            else:
                @pl.when(c >= 2)
                def _():
                    put(r, c - 2, slot).wait()

                @pl.when(c < 2)
                def _():
                    put(before, n_cols - 2 + c, slot).wait()
            rows = jnp.dot(pick[...], u_buf[r, :, cols], preferred_element_type=jnp.float32).astype(jnp.bfloat16)
            for e in range(local):
                stage[slot, e] = rows[e * capacity:(e + 1) * capacity, :]
            put(r, c, slot).start()

    dispatch(0, None)
    tokens.arrive(tokens.mate)
    dispatch(4, 0)
    tokens.forward()
    dispatch(1, 4)
    dispatch(2, 1)
    tokens.arrive(tokens.near_mate)
    dispatch(5, 2)
    tokens.forward_far()
    dispatch(6, 5)
    dispatch(3, 6)
    tokens.arrive(tokens.far_mate)
    dispatch(7, 3)
    gates.arrive(gates.own + gates.mate)
    for copy in gates.near_mate:
        copy.start()
    gates.forward_far()
    gates.arrive(gates.near_mate + gates.far_mate)
    for r in range(group):
        gates_ref[r] = g_buf[r]
    for c in range(n_cols - 2, n_cols):
        put(7, c, c % 2).wait()
    tokens.finish()
    gates.finish()


def dispatch_tokens(h, router_t, ids_t, rank, capacity):
    n_tok, d_model = h.shape
    group, local = rank.shape[:2]
    top_k = ids_t.shape[0]
    width = 512
    vmem = pl.BlockSpec(memory_space=pltpu.VMEM)
    return pl.pallas_call(
        dispatch_kernel,
        in_specs=[vmem] * 4,
        out_specs=[pl.BlockSpec(memory_space=pl.ANY), vmem],
        out_shape=[jax.ShapeDtypeStruct((group, local, capacity, d_model), jnp.bfloat16), jax.ShapeDtypeStruct((group, top_k, n_tok), jnp.float32)],
        scratch_shapes=[
            pltpu.VMEM((group, n_tok, d_model), jnp.bfloat16),
            pltpu.VMEM((local * capacity, n_tok), jnp.bfloat16),
            pltpu.VMEM((2, local, capacity, width), jnp.bfloat16),
            pltpu.VMEM((group, top_k, n_tok), jnp.float32),
            pltpu.SemaphoreType.DMA((2,)),
            pltpu.SemaphoreType.DMA((9,)),
            pltpu.SemaphoreType.DMA((9,)),
            pltpu.SemaphoreType.DMA((9,)),
            pltpu.SemaphoreType.DMA((9,)),
        ],
        compiler_params=pltpu.CompilerParams(vmem_limit_bytes=MAX_VMEM, collective_id=1, has_side_effects=True),
        cost_estimate=pl.CostEstimate(flops=2 * group * local * capacity * n_tok * d_model, bytes_accessed=2 * group * local * capacity * d_model, transcendentals=0),
        name="dispatch_tokens",
    )(h, router_t, ids_t, rank)


def expert_kernel(size_ref, start_ref, total_ref, x_ref, gate_ref, up_ref, down_ref, f_ref, x_buf, f_buf, in_sems, out_sems, *, chunk):
    n_src, _, capacity, d_model = x_ref.shape
    e, local = pl.program_id(0), pl.num_programs(0)
    slot = lax.rem(e, 2)
    zeros = jnp.zeros((capacity, d_model), jnp.bfloat16)

    def fetch(r, expert, where):
        size = pl.multiple_of(size_ref[r, expert], ALIGN)
        start = pl.multiple_of(start_ref[r, expert], ALIGN)
        return pltpu.make_async_copy(x_ref.at[r, expert, pl.ds(0, size), :], x_buf.at[where, pl.ds(start, size), :], in_sems.at[where, r])

    def put(r, expert, where):
        start = pl.multiple_of(start_ref[r, expert], ALIGN)
        return pltpu.make_async_copy(f_buf.at[where, pl.ds(start, capacity), :], f_ref.at[r, expert], out_sems.at[where, r])

    @pl.when(e == 0)
    def _():
        for r in range(n_src):
            fetch(r, 0, 0).start()

    @pl.when(e + 1 < local)
    def _():
        for r in range(n_src):
            fetch(r, e + 1, 1 - slot).start()

    for r in range(n_src):
        fetch(r, e, slot).wait()

    @pl.when(e >= 2)
    def _():
        for r in range(n_src):
            put(r, e - 2, slot).wait()

    total = total_ref[e]
    x_buf[slot, pl.ds(pl.multiple_of(total, ALIGN), capacity), :] = zeros
    chunks = (total + chunk - 1) // chunk

    @pl.loop(0, chunks)
    def _(i):
        rows = pl.ds(pl.multiple_of(i * chunk, chunk), chunk)
        x = x_buf[slot, rows, :]
        gate_act = jnp.dot(x, gate_ref[0], preferred_element_type=jnp.float32)
        up_act = jnp.dot(x, up_ref[0], preferred_element_type=jnp.float32)
        middle = (gate_act * jax.nn.sigmoid(gate_act) * up_act).astype(jnp.bfloat16)
        f_buf[slot, rows, :] = jnp.dot(middle, down_ref[0], preferred_element_type=jnp.float32).astype(jnp.bfloat16)

    f_buf[slot, pl.ds(pl.multiple_of(chunks * chunk, chunk), capacity), :] = zeros
    for r in range(n_src):
        put(r, e, slot).start()

    @pl.when(e == local - 1)
    def _():
        @pl.when(e >= 1)
        def _():
            for r in range(n_src):
                put(r, e - 1, 1 - slot).wait()
        for r in range(n_src):
            put(r, e, slot).wait()


def experts(sizes, starts, totals, rows, gate_w, up_w, down_w):
    n_src, local, capacity, d_model = rows.shape
    width = gate_w.shape[2]
    chunk = capacity
    n_rows = n_src * capacity + 2 * capacity
    anywhere = pl.BlockSpec(memory_space=pl.ANY)
    return pl.pallas_call(
        functools.partial(expert_kernel, chunk=chunk),
        grid_spec=pltpu.PrefetchScalarGridSpec(
            num_scalar_prefetch=3,
            grid=(local,),
            in_specs=[anywhere] + [
                pl.BlockSpec((1, d_model, width), lambda e, *_: (e, 0, 0)),
                pl.BlockSpec((1, d_model, width), lambda e, *_: (e, 0, 0)),
                pl.BlockSpec((1, width, d_model), lambda e, *_: (e, 0, 0)),
            ],
            out_specs=anywhere,
            scratch_shapes=[
                pltpu.VMEM((2, n_rows, d_model), jnp.bfloat16),
                pltpu.VMEM((2, n_rows, d_model), jnp.bfloat16),
                pltpu.SemaphoreType.DMA((2, n_src)),
                pltpu.SemaphoreType.DMA((2, n_src)),
            ],
        ),
        out_shape=jax.ShapeDtypeStruct(rows.shape, jnp.bfloat16),
        compiler_params=params(),
        cost_estimate=pl.CostEstimate(flops=4 * local * n_src * capacity * d_model * width, bytes_accessed=6 * local * d_model * width, transcendentals=0),
        name="experts",
    )(sizes, starts, totals, rows, gate_w, up_w, down_w)


def reduce_kernel(rank_ref, piece_ref, f_ref, out_ref, f_buf, spread, other_buf, swap_buf, send_buf, ring_buf, f_sems, swap_send, swap_recv, ring_send, ring_recv, out_sems, free_sem):
    n_src, n_tok, local = rank_ref.shape
    capacity = f_ref.shape[2]
    pieces = piece_ref.shape[2] // local
    chips = n_src // 2
    width = out_ref.shape[1] // 4
    n_units = 16

    def quarter(u):
        return 2 * lax.rem(u, 2) + u // 2

    def place(i):
        u = lax.rem(i, 4)
        odd = lax.rem(u, 2)
        target = jnp.where(i < 4, 1 + odd, jnp.where(i < 8, 2 - odd, jnp.where(i < 12, 3, 0)))
        return u, target

    def fetch(i, side, slot):
        u, target = place(i)
        cols = pl.ds(pl.multiple_of(quarter(u) * width, width), width)
        return pltpu.make_async_copy(f_ref.at[target + chips * (1 - side), :, :, cols], f_buf.at[slot, side], f_sems.at[slot, side])

    def swap_copy(i):
        s = lax.rem(i, 4)
        return remote(other_buf.at[s], swap_buf.at[s], swap_send.at[s], swap_recv.at[s], neighbour(0, True))

    def ring_copy(source, slot):
        return remote(send_buf.at[source], ring_buf.at[slot], ring_send.at[slot], ring_recv.at[slot], neighbour(1 - 2 * lax.rem(slot, 2)))

    def build(target, entry):
        @pl.loop(0, 2)
        def _(side):
            r = target + chips * (1 - side)
            rank = rank_ref[r]
            weights = piece_ref[r]
            slots = lax.broadcasted_iota(jnp.int32, (n_tok, capacity), 1)
            for e in range(local):
                hit = rank[:, e:e + 1] == slots
                for k in range(pieces):
                    column = k * local + e
                    spread[entry * 2 + side, k, :, e * capacity:(e + 1) * capacity] = jnp.where(hit, weights[:, column:column + 1], 0.0).astype(jnp.bfloat16)

    def product(entry, slot, side):
        data = jnp.concatenate([f_buf[slot, side, e] for e in range(local)], axis=0)
        total = jnp.dot(spread[entry * 2 + side, 0], data, preferred_element_type=jnp.float32)
        for k in range(1, pieces):
            total += jnp.dot(spread[entry * 2 + side, k], data, preferred_element_type=jnp.float32)
        return total

    for side in range(2):
        fetch(0, side, 0).start()
    greet(neighbour(1), neighbour(-1), neighbour(0, True))

    @pl.loop(0, n_units)
    def _(i):
        u, target = place(i)
        slot = lax.rem(i, 2)
        lane = lax.rem(i, 4)

        @pl.when(i + 1 < n_units)
        def _():
            for side in range(2):
                fetch(i + 1, side, 1 - slot).start()

        @pl.when(i == 0)
        def _():
            build(1, 0)

        @pl.when(i == 1)
        def _():
            build(2, 1)

        @pl.when(i == 8)
        def _():
            build(3, 0)

        @pl.when(i == 12)
        def _():
            build(0, 1)

        entry = 1 - lax.rem(target, 2)

        @pl.when(i >= 4)
        def _():
            swap_copy(i - 4).wait_send()
            pl.semaphore_wait(free_sem, 1)

        fetch(i, 0, slot).wait()
        other_buf[lane] = product(entry, slot, 0)
        swap_copy(i).start()
        fetch(i, 1, slot).wait()
        send_buf[i] = product(entry, slot, 1)
        swap_copy(i).wait_recv()
        send_buf[i] += swap_buf[lane]

        @pl.when(i < n_units - 4)
        def _():
            pl.semaphore_signal(free_sem, inc=1, device_id=neighbour(0, True), device_id_type=pl.DeviceIdType.MESH)

        @pl.when(i < 4)
        def _():
            ring_copy(i, u).start()

        @pl.when((i >= 8) & (i < 12))
        def _():
            ring_copy(i, u).wait_recv()
            send_buf[i] += ring_buf[u]
            ring_copy(i, u + 4).start()

    @pl.loop(0, 4)
    def _(u):
        ring_copy(0, u + 4).wait_recv()
        send_buf[u + 4] += ring_buf[u + 4]
        ring_copy(u + 4, u + 8).start()

    def put(u):
        cols = pl.ds(pl.multiple_of(quarter(u) * width, width), width)
        return pltpu.make_async_copy(send_buf.at[12 + u], out_ref.at[:, cols], out_sems.at[u])

    @pl.loop(0, 4)
    def _(u):
        ring_copy(0, u + 8).wait_recv()
        send_buf[12 + u] += ring_buf[u + 8]
        put(u).start()

    @pl.loop(0, 4)
    def _(u):
        put(u).wait()
        swap_copy(n_units - 4 + u).wait_send()
        ring_copy(u, u).wait_send()
        ring_copy(8 + u, u + 4).wait_send()
        ring_copy(4 + u, u + 8).wait_send()


def reduce_results(rank_t, pieces, results):
    n_src, local, capacity, d_model = results.shape
    n_tok = rank_t.shape[1]
    width = d_model // 4
    n_pieces = pieces.shape[2] // local
    tile = (n_tok, width)
    vmem = pl.BlockSpec(memory_space=pltpu.VMEM)
    return pl.pallas_call(
        reduce_kernel,
        in_specs=[vmem, vmem, pl.BlockSpec(memory_space=pl.ANY)],
        out_specs=pl.BlockSpec(memory_space=pl.ANY),
        out_shape=jax.ShapeDtypeStruct((n_tok, d_model), jnp.float32),
        scratch_shapes=[
            pltpu.VMEM((2, 2, local, capacity, width), jnp.bfloat16),
            pltpu.VMEM((4, n_pieces, n_tok, local * capacity), jnp.bfloat16),
            pltpu.VMEM((4,) + tile, jnp.float32),
            pltpu.VMEM((4,) + tile, jnp.float32),
            pltpu.VMEM((16,) + tile, jnp.float32),
            pltpu.VMEM((12,) + tile, jnp.float32),
            pltpu.SemaphoreType.DMA((2, 2)),
            pltpu.SemaphoreType.DMA((4,)),
            pltpu.SemaphoreType.DMA((4,)),
            pltpu.SemaphoreType.DMA((12,)),
            pltpu.SemaphoreType.DMA((12,)),
            pltpu.SemaphoreType.DMA((4,)),
            pltpu.SemaphoreType.REGULAR,
        ],
        compiler_params=pltpu.CompilerParams(vmem_limit_bytes=MAX_VMEM, collective_id=2, has_side_effects=True),
        cost_estimate=pl.CostEstimate(flops=6 * n_src * local * capacity * n_tok * d_model, bytes_accessed=4 * n_src * local * capacity * d_model, transcendentals=0),
        name="reduce_results",
    )(rank_t, pieces, results)


def bf16_pieces(values):
    first = lax.reduce_precision(values, 8, 7)
    second = lax.reduce_precision(values - first, 8, 7)
    third = values - first - second
    return first, second, third


def local_layer(x_loc, q_shard, k_shard, v_shard, o_shard, w_router, gate_loc, up_loc, down_loc, sgate_shard, sup_shard, sdown_shard, ids_loc, group):
    n_seq, seq_len, d_model = x_loc.shape
    assert n_seq == 1 and group == 8 and q_shard.shape[2] == 128
    n_tok = n_seq * seq_len
    top_k = ids_loc.shape[-1]
    local = gate_loc.shape[0]
    n_experts = local * group
    capacity = CAP_FACTOR * n_tok * top_k // n_experts
    def gathered(shard):
        return lax.all_gather(shard.reshape(shard.shape[0], -1), 'ep', axis=0, tiled=True)

    def project(rows, weight):
        return jnp.dot(rows, weight, preferred_element_type=jnp.float32).astype(jnp.bfloat16)

    x_flat = x_loc.reshape(n_tok, d_model)
    ids_t = ids_loc.reshape(n_tok, top_k).T
    residual, rank, ids_all = attention_layer(x_flat, ids_t, *[w.reshape(w.shape[0], -1) for w in (k_shard, v_shard, q_shard, o_shard)], group, local)
    rows, gates_all = dispatch_tokens(residual, w_router.T, ids_t, rank, capacity)

    rank_t = rank.transpose(0, 2, 1)
    sizes = (jnp.max(rank, axis=2) + 1 + ALIGN - 1) // ALIGN * ALIGN
    ends = jnp.cumsum(sizes, axis=0)
    starts, totals = ends - sizes, ends[-1]
    rows, sgate_shard, sup_shard, sdown_shard = lax.optimization_barrier((rows, sgate_shard, sup_shard, sdown_shard))
    results = experts(sizes, starts, totals, rows, gate_loc, up_loc, down_loc)

    mine = lax.axis_index('ep') * local + jnp.arange(local)
    chosen = ids_all[:, None, :, :] == mine[None, :, None, None]
    weight = jnp.sum(jnp.where(chosen, gates_all[:, None, :, :], 0.0), axis=2)
    pieces = jnp.concatenate(bf16_pieces(weight), axis=1).transpose(0, 2, 1)

    moe_in = rms_norm(residual).astype(jnp.bfloat16)
    gate_act = jnp.dot(moe_in, gathered(sgate_shard), preferred_element_type=jnp.float32)
    up_act = jnp.dot(moe_in, gathered(sup_shard), preferred_element_type=jnp.float32)
    middle = (jax.nn.silu(gate_act) * up_act).astype(jnp.bfloat16)
    shared = project(middle, gathered(sdown_shard))
    routed = reduce_results(rank_t, pieces, results)
    y_out = (residual.astype(jnp.float32) + routed + shared.astype(jnp.float32)).astype(jnp.bfloat16)
    return y_out.reshape(n_seq, seq_len, d_model)


def solution(mesh):
    tok_spec = P(('dp', 'ep'), None, None)
    row_spec = P('ep', None)
    cube_spec = P('ep', None, None)
    in_specs = (tok_spec, cube_spec, cube_spec, cube_spec, row_spec, P(None, None), cube_spec, cube_spec, cube_spec, row_spec, row_spec, row_spec, tok_spec)
    return jax.shard_map(functools.partial(local_layer, group=mesh.shape['ep']), mesh=mesh, in_specs=in_specs, out_specs=tok_spec, check_vma=False)
```

```python
import functools
import jax
import jax.numpy as jnp
from jax import lax
from jax.experimental import pallas as pl
from jax.experimental.pallas import tpu as pltpu
from jax.sharding import PartitionSpec as P

EPSILON = 1e-6
CAP_FACTOR = 2
ALIGN = 16
VMEM_BYTES = 60 * 1024 * 1024
MAX_VMEM = 67043328


def rms_norm(values):
    as_f32 = values.astype(jnp.float32)
    return as_f32 * lax.rsqrt(jnp.mean(as_f32 * as_f32, axis=-1, keepdims=True) + EPSILON)


def params(**kw):
    return pltpu.CompilerParams(vmem_limit_bytes=VMEM_BYTES, **kw)


def neighbour(chips, swap=False):
    me, group = lax.axis_index('ep'), lax.axis_size('ep')
    side = lax.rem(me, 2)
    chip = lax.rem(me // 2 + chips + group // 2, group // 2)
    return {'ep': chip * 2 + (1 - side if swap else side)}


def greet(*devices):
    barrier = pltpu.get_barrier_semaphore()
    for device in devices:
        pl.semaphore_signal(barrier, inc=1, device_id=device, device_id_type=pl.DeviceIdType.MESH)
    pl.semaphore_wait(barrier, len(devices))


def remote(src, dst, send_sem, recv_sem, device):
    return pltpu.make_async_remote_copy(src_ref=src, dst_ref=dst, send_sem=send_sem, recv_sem=recv_sem, device_id=device, device_id_type=pl.DeviceIdType.MESH)


class Gather:
    def __init__(self, buf, send, recv, split=True):
        other = neighbour(0, True)
        half = buf.shape[1] // 2
        lo, hi = pl.ds(0, half), pl.ds(half, half)

        def copy(k, src, dst, device):
            return remote(src, dst, send.at[k], recv.at[k], device)

        self.own = [copy(0, buf.at[0], buf.at[1], neighbour(1)), copy(1, buf.at[0], buf.at[2], neighbour(-1))]
        self.mate = [copy(2, buf.at[0], buf.at[4], other)]
        self.near_mate = [copy(3, buf.at[1], buf.at[5], other), copy(4, buf.at[2], buf.at[6], other)]
        if split:
            self.far = [copy(5, buf.at[1, lo], buf.at[3, lo], neighbour(1)), copy(6, buf.at[2, hi], buf.at[3, hi], neighbour(-1))]
            self.far_mate = [copy(7, buf.at[3, lo], buf.at[7, lo], other), copy(8, buf.at[3, hi], buf.at[7, hi], other)]
        else:
            self.far = [copy(5, buf.at[0], buf.at[3], neighbour(2))]
            self.far_mate = [copy(7, buf.at[3], buf.at[7], other)]
        self.split = split

    def begin(self):
        for copy in self.own + self.mate + ([] if self.split else self.far):
            copy.start()

    def forward(self):
        for k in range(2):
            self.own[k].wait_recv()
            if self.split:
                self.far[k].start()
            self.near_mate[k].start()

    def forward_far(self):
        for copy, mate in zip(self.far, self.far_mate):
            copy.wait_recv()
            mate.start()

    def arrive(self, copies):
        for copy in copies:
            copy.wait_recv()

    def finish(self):
        for copy in self.own + self.mate + self.near_mate + self.far + self.far_mate:
            copy.wait_send()


def owner(r):
    step = (0, -1, 1, 2)[r % 4]
    return neighbour(step, r >= 4)['ep']


def attention_layer_kernel(x_ref, ids_ref, k_hbm, v_hbm, q_hbm, o_hbm, h_ref, rank_ref, ids_out, w_buf, n_buf, qkv, ids_buf, load_sems, send, recv, ids_send, ids_recv):
    n_tok, d_model = x_ref.shape
    group, local = rank_ref.shape[:2]
    size = d_model // group
    head = 128
    width = 512
    keys, vals, queries, outs = range(4)
    gathers = [Gather(w_buf.at[w], send.at[w], recv.at[w]) for w in range(4)]
    ids_gather = Gather(ids_buf, ids_send, ids_recv, split=False)
    loads = [pltpu.make_async_copy(ref, w_buf.at[w, 0], load_sems.at[w]) for w, ref in enumerate((k_hbm, v_hbm, q_hbm, o_hbm))]
    ids_load = pltpu.make_async_copy(ids_ref, ids_buf.at[0], load_sems.at[4])
    ids_load.start()
    for load in loads:
        load.start()
    greet(neighbour(1), neighbour(-1), neighbour(2), neighbour(0, True))
    ids_load.wait()
    ids_gather.begin()
    for w in (keys, vals):
        loads[w].wait()
        gathers[w].begin()

    @pl.loop(0, n_tok // 128)
    def _(i):
        rows = pl.ds(pl.multiple_of(i * 128, 128), 128)
        normed = rms_norm(x_ref[rows, :]).astype(jnp.bfloat16)
        qkv[0, rows, :] = normed
        for r in range(group):
            n_buf[rows, r * size:(r + 1) * size] = qkv[0, rows, pl.ds(pl.multiple_of(owner(r) * size, size), size)]

    ids_gather.arrive(ids_gather.own + ids_gather.mate)
    for copy in ids_gather.near_mate:
        copy.start()
    ids_gather.forward_far()
    ids_gather.arrive(ids_gather.near_mate + ids_gather.far_mate)
    first = lax.axis_index('ep') * local
    before = (lax.broadcasted_iota(jnp.int32, (n_tok, n_tok), 0) < lax.broadcasted_iota(jnp.int32, (n_tok, n_tok), 1)).astype(jnp.float32).astype(jnp.bfloat16)
    for r in range(group):
        member = jnp.concatenate([jnp.max((ids_buf[r] == first + e).astype(jnp.float32), axis=0, keepdims=True) for e in range(local)], axis=0)
        rank = jnp.dot(member.astype(jnp.bfloat16), before, preferred_element_type=jnp.float32)
        rank_ref[r] = jnp.where(member > 0.5, rank, -1.0).astype(jnp.int32)

    def project(w, store):
        @pl.loop(0, d_model // width)
        def _(c):
            cols = pl.ds(pl.multiple_of(c * width, width), width)
            weight = jnp.concatenate([w_buf[w, r, :, cols] for r in range(group)], axis=0)
            store(cols, jnp.dot(n_buf[...], weight, preferred_element_type=jnp.float32).astype(jnp.bfloat16))

    def keep(w):
        def store(cols, values):
            qkv[w, :, cols] = values
        return store

    def complete(w):
        gathers[w].forward_far()
        gathers[w].arrive(gathers[w].mate + gathers[w].near_mate + gathers[w].far_mate)

    def attend(lo, hi):
        for r in range(lo, hi):
            start = owner(r) * size

            @pl.loop(0, size // head)
            def _(k):
                cols = pl.ds(pl.multiple_of(start + k * head, head), head)
                parts = 2
                step = n_tok // parts
                for part in range(parts):
                    top, end = part * step, (part + 1) * step
                    scores = lax.dot_general(qkv[queries, top:end, cols], qkv[keys, :end, cols], (((1,), (1,)), ((), ())), preferred_element_type=jnp.float32) * (head ** -0.5)
                    row = top + lax.broadcasted_iota(jnp.int32, scores.shape, 0)
                    col = lax.broadcasted_iota(jnp.int32, scores.shape, 1)
                    scores = jnp.where(row >= col, scores, -1e30)
                    weights = jnp.exp(scores - jnp.max(scores, axis=-1, keepdims=True))
                    probs = (weights / jnp.sum(weights, axis=-1, keepdims=True)).astype(jnp.bfloat16)
                    n_buf[top:end, pl.ds(pl.multiple_of(r * size + k * head, head), head)] = jnp.dot(probs, qkv[vals, :end, cols], preferred_element_type=jnp.float32).astype(jnp.bfloat16)

    gathers[keys].forward()
    loads[queries].wait()
    gathers[queries].begin()
    gathers[vals].forward()
    complete(keys)
    project(keys, keep(keys))
    gathers[queries].forward()
    loads[outs].wait()
    gathers[outs].begin()
    complete(vals)
    project(vals, keep(vals))
    complete(queries)
    project(queries, keep(queries))
    attend(0, group // 2)
    gathers[outs].forward()
    attend(group // 2, group)
    complete(outs)

    def residual(cols, values):
        h_ref[:, cols] = (x_ref[:, cols].astype(jnp.float32) + values.astype(jnp.float32)).astype(jnp.bfloat16)

    project(outs, residual)
    for r in range(group):
        ids_out[r] = ids_buf[r]
    for gather in gathers + [ids_gather]:
        gather.finish()


def attention_layer(x, ids_t, k_shard, v_shard, q_shard, o_shard, group, local):
    n_tok, d_model = x.shape
    top_k = ids_t.shape[0]
    vmem = pl.BlockSpec(memory_space=pltpu.VMEM)
    anywhere = pl.BlockSpec(memory_space=pl.ANY)
    return pl.pallas_call(
        attention_layer_kernel,
        in_specs=[vmem] + [anywhere] * 5,
        out_specs=[vmem] * 3,
        out_shape=[jax.ShapeDtypeStruct(x.shape, jnp.bfloat16), jax.ShapeDtypeStruct((group, local, n_tok), jnp.int32), jax.ShapeDtypeStruct((group, top_k, n_tok), jnp.int32)],
        scratch_shapes=[
            pltpu.VMEM((4, group) + k_shard.shape, jnp.bfloat16),
            pltpu.VMEM(x.shape, jnp.bfloat16),
            pltpu.VMEM((3,) + x.shape, jnp.bfloat16),
            pltpu.VMEM((group, top_k, n_tok), jnp.int32),
            pltpu.SemaphoreType.DMA((5,)),
            pltpu.SemaphoreType.DMA((4, 9)),
            pltpu.SemaphoreType.DMA((4, 9)),
            pltpu.SemaphoreType.DMA((9,)),
            pltpu.SemaphoreType.DMA((9,)),
        ],
        compiler_params=pltpu.CompilerParams(vmem_limit_bytes=MAX_VMEM, collective_id=0, has_side_effects=True),
        cost_estimate=pl.CostEstimate(flops=9 * n_tok * d_model * d_model, bytes_accessed=8 * d_model * d_model // group, transcendentals=0),
        name="attention_layer",
    )(x, ids_t, k_shard, v_shard, q_shard, o_shard)


def dispatch_kernel(h_ref, wr_ref, ids_ref, rank_ref, x_hbm, gates_ref, u_hbm, u_buf, pick, stage, g_buf, out_sems, send, recv, g_send, g_recv):
    n_tok, d_model = h_ref.shape
    group, local = rank_ref.shape[:2]
    capacity = x_hbm.shape[2]
    n_experts = wr_ref.shape[0]
    top_k = ids_ref.shape[0]
    width = stage.shape[3]
    n_cols = d_model // width
    tokens = Gather(u_buf, send, recv)
    gates = Gather(g_buf, g_send, g_recv, split=False)

    @pl.loop(0, n_tok // 128)
    def _(i):
        rows = pl.ds(pl.multiple_of(i * 128, 128), 128)
        u_buf[0, rows, :] = rms_norm(h_ref[rows, :]).astype(jnp.bfloat16)

    greet(neighbour(1), neighbour(-1), neighbour(2), neighbour(0, True))
    tokens.begin()
    keep = pltpu.make_async_copy(u_buf.at[0], u_hbm, out_sems.at[2])
    keep.start()

    for i in range(n_tok // 128):
        rows = slice(i * 128, (i + 1) * 128)
        logits = lax.dot_general(wr_ref[...], rms_norm(h_ref[rows, :]), (((1,), (1,)), ((), ())), precision=lax.Precision.HIGHEST, preferred_element_type=jnp.float32)
        experts_iota = lax.broadcasted_iota(jnp.int32, (n_experts, 128), 0)
        chosen = jnp.concatenate([jnp.sum(jnp.where(experts_iota == ids_ref[j:j + 1, rows], logits, 0.0), axis=0, keepdims=True) for j in range(top_k)], axis=0)
        weights = jnp.exp(chosen - jnp.max(chosen, axis=0, keepdims=True))
        g_buf[0, :, rows] = weights / jnp.sum(weights, axis=0, keepdims=True)
    gates.begin()

    def put(r, c, slot):
        cols = pl.ds(pl.multiple_of(c * width, width), width)
        return pltpu.make_async_copy(stage.at[slot], x_hbm.at[r, :, :, cols], out_sems.at[slot])

    def dispatch(r, before):
        slots = lax.broadcasted_iota(jnp.int32, (capacity, n_tok), 0)
        for e in range(local):
            pick[e * capacity:(e + 1) * capacity, :] = (rank_ref[r, e:e + 1, :] == slots).astype(jnp.float32).astype(jnp.bfloat16)

        @pl.loop(0, n_cols)
        def _(c):
            slot = lax.rem(c, 2)
            cols = pl.ds(pl.multiple_of(c * width, width), width)
            if before is None:
                @pl.when(c >= 2)
                def _():
                    put(r, c - 2, slot).wait()
            else:
                @pl.when(c >= 2)
                def _():
                    put(r, c - 2, slot).wait()

                @pl.when(c < 2)
                def _():
                    put(before, n_cols - 2 + c, slot).wait()
            rows = jnp.dot(pick[...], u_buf[r, :, cols], preferred_element_type=jnp.float32).astype(jnp.bfloat16)
            for e in range(local):
                stage[slot, e] = rows[e * capacity:(e + 1) * capacity, :]
            put(r, c, slot).start()

    dispatch(0, None)
    tokens.arrive(tokens.mate)
    dispatch(4, 0)
    tokens.forward()
    dispatch(1, 4)
    dispatch(2, 1)
    tokens.arrive(tokens.near_mate)
    dispatch(5, 2)
    tokens.forward_far()
    dispatch(6, 5)
    dispatch(3, 6)
    tokens.arrive(tokens.far_mate)
    dispatch(7, 3)
    gates.arrive(gates.own + gates.mate)
    for copy in gates.near_mate:
        copy.start()
    gates.forward_far()
    gates.arrive(gates.near_mate + gates.far_mate)
    for r in range(group):
        gates_ref[r] = g_buf[r]
    for c in range(n_cols - 2, n_cols):
        put(7, c, c % 2).wait()
    keep.wait()
    tokens.finish()
    gates.finish()


def dispatch_tokens(h, router_t, ids_t, rank, capacity):
    n_tok, d_model = h.shape
    group, local = rank.shape[:2]
    top_k = ids_t.shape[0]
    width = 512
    vmem = pl.BlockSpec(memory_space=pltpu.VMEM)
    return pl.pallas_call(
        dispatch_kernel,
        in_specs=[vmem] * 4,
        out_specs=[pl.BlockSpec(memory_space=pl.ANY), vmem, pl.BlockSpec(memory_space=pl.ANY)],
        out_shape=[jax.ShapeDtypeStruct((group, local, capacity, d_model), jnp.bfloat16), jax.ShapeDtypeStruct((group, top_k, n_tok), jnp.float32), jax.ShapeDtypeStruct(h.shape, jnp.bfloat16)],
        scratch_shapes=[
            pltpu.VMEM((group, n_tok, d_model), jnp.bfloat16),
            pltpu.VMEM((local * capacity, n_tok), jnp.bfloat16),
            pltpu.VMEM((2, local, capacity, width), jnp.bfloat16),
            pltpu.VMEM((group, top_k, n_tok), jnp.float32),
            pltpu.SemaphoreType.DMA((3,)),
            pltpu.SemaphoreType.DMA((9,)),
            pltpu.SemaphoreType.DMA((9,)),
            pltpu.SemaphoreType.DMA((9,)),
            pltpu.SemaphoreType.DMA((9,)),
        ],
        compiler_params=pltpu.CompilerParams(vmem_limit_bytes=MAX_VMEM, collective_id=1, has_side_effects=True),
        cost_estimate=pl.CostEstimate(flops=2 * group * local * capacity * n_tok * d_model, bytes_accessed=2 * group * local * capacity * d_model, transcendentals=0),
        name="dispatch_tokens",
    )(h, router_t, ids_t, rank)


def expert_kernel(size_ref, start_ref, total_ref, x_ref, gate_ref, up_ref, down_ref, f_ref, x_buf, f_buf, in_sems, out_sems, *, chunk):
    n_src, _, capacity, d_model = x_ref.shape
    e, local = pl.program_id(0), pl.num_programs(0)
    slot = lax.rem(e, 2)
    zeros = jnp.zeros((capacity, d_model), jnp.bfloat16)

    def fetch(r, expert, where):
        size = pl.multiple_of(size_ref[r, expert], ALIGN)
        start = pl.multiple_of(start_ref[r, expert], ALIGN)
        return pltpu.make_async_copy(x_ref.at[r, expert, pl.ds(0, size), :], x_buf.at[where, pl.ds(start, size), :], in_sems.at[where, r])

    def put(r, expert, where):
        start = pl.multiple_of(start_ref[r, expert], ALIGN)
        return pltpu.make_async_copy(f_buf.at[where, pl.ds(start, capacity), :], f_ref.at[r, expert], out_sems.at[where, r])

    @pl.when(e == 0)
    def _():
        for r in range(n_src):
            fetch(r, 0, 0).start()

    @pl.when(e + 1 < local)
    def _():
        for r in range(n_src):
            fetch(r, e + 1, 1 - slot).start()

    for r in range(n_src):
        fetch(r, e, slot).wait()

    @pl.when(e >= 2)
    def _():
        for r in range(n_src):
            put(r, e - 2, slot).wait()

    total = total_ref[e]
    x_buf[slot, pl.ds(pl.multiple_of(total, ALIGN), capacity), :] = zeros
    chunks = (total + chunk - 1) // chunk

    def run(start, size):
        rows = pl.ds(pl.multiple_of(start, chunk), size)
        x = x_buf[slot, rows, :]
        gate_act = jnp.dot(x, gate_ref[0], preferred_element_type=jnp.float32)
        up_act = jnp.dot(x, up_ref[0], preferred_element_type=jnp.float32)
        middle = (gate_act * jax.nn.sigmoid(gate_act) * up_act).astype(jnp.bfloat16)
        f_buf[slot, rows, :] = jnp.dot(middle, down_ref[0], preferred_element_type=jnp.float32).astype(jnp.bfloat16)

    @pl.loop(0, chunks // 2)
    def _(i):
        run(i * 2 * chunk, 2 * chunk)

    @pl.when(lax.rem(chunks, 2) == 1)
    def _():
        run((chunks - 1) * chunk, chunk)

    f_buf[slot, pl.ds(pl.multiple_of(chunks * chunk, chunk), capacity), :] = zeros
    for r in range(n_src):
        put(r, e, slot).start()

    @pl.when(e == local - 1)
    def _():
        @pl.when(e >= 1)
        def _():
            for r in range(n_src):
                put(r, e - 1, 1 - slot).wait()
        for r in range(n_src):
            put(r, e, slot).wait()


def experts(sizes, starts, totals, rows, gate_w, up_w, down_w):
    n_src, local, capacity, d_model = rows.shape
    width = gate_w.shape[2]
    chunk = capacity
    n_rows = n_src * capacity + 2 * capacity
    anywhere = pl.BlockSpec(memory_space=pl.ANY)
    return pl.pallas_call(
        functools.partial(expert_kernel, chunk=chunk),
        grid_spec=pltpu.PrefetchScalarGridSpec(
            num_scalar_prefetch=3,
            grid=(local,),
            in_specs=[anywhere] + [
                pl.BlockSpec((1, d_model, width), lambda e, *_: (e, 0, 0)),
                pl.BlockSpec((1, d_model, width), lambda e, *_: (e, 0, 0)),
                pl.BlockSpec((1, width, d_model), lambda e, *_: (e, 0, 0)),
            ],
            out_specs=anywhere,
            scratch_shapes=[
                pltpu.VMEM((2, n_rows, d_model), jnp.bfloat16),
                pltpu.VMEM((2, n_rows, d_model), jnp.bfloat16),
                pltpu.SemaphoreType.DMA((2, n_src)),
                pltpu.SemaphoreType.DMA((2, n_src)),
            ],
        ),
        out_shape=jax.ShapeDtypeStruct(rows.shape, jnp.bfloat16),
        compiler_params=params(),
        cost_estimate=pl.CostEstimate(flops=4 * local * n_src * capacity * d_model * width, bytes_accessed=6 * local * d_model * width, transcendentals=0),
        name="experts",
    )(sizes, starts, totals, rows, gate_w, up_w, down_w)


def reduce_kernel(rank_ref, piece_ref, f_ref, h_hbm, u_hbm, gate_hbm, up_hbm, down_hbm, out_ref, f_buf, spread, other_buf, swap_buf, send_buf, ring_buf, f_sems, swap_send, swap_recv, ring_send, ring_recv, out_sems, free_sem):
    n_src, n_tok, local = rank_ref.shape
    capacity = f_ref.shape[2]
    pieces = piece_ref.shape[2] // local
    chips = n_src // 2
    width = out_ref.shape[1] // 4
    n_units = 16

    def quarter(u):
        return 2 * lax.rem(u, 2) + u // 2

    def place(i):
        u = lax.rem(i, 4)
        odd = lax.rem(u, 2)
        target = jnp.where(i < 4, 1 + odd, jnp.where(i < 8, 2 - odd, jnp.where(i < 12, 3, 0)))
        return u, target

    def fetch(i, side, slot):
        u, target = place(i)
        cols = pl.ds(pl.multiple_of(quarter(u) * width, width), width)
        return pltpu.make_async_copy(f_ref.at[target + chips * (1 - side), :, :, cols], f_buf.at[slot, side], f_sems.at[slot, side])

    def swap_copy(i):
        s = lax.rem(i, 4)
        return remote(other_buf.at[s], swap_buf.at[s], swap_send.at[s], swap_recv.at[s], neighbour(0, True))

    def ring_copy(source, slot):
        return remote(send_buf.at[source], ring_buf.at[slot], ring_send.at[slot], ring_recv.at[slot], neighbour(1 - 2 * lax.rem(slot, 2)))

    def build(target, entry):
        @pl.loop(0, 2)
        def _(side):
            r = target + chips * (1 - side)
            rank = rank_ref[r]
            weights = piece_ref[r]
            slots = lax.broadcasted_iota(jnp.int32, (n_tok, capacity), 1)
            for e in range(local):
                hit = rank[:, e:e + 1] == slots
                for k in range(pieces):
                    column = k * local + e
                    spread[entry * 2 + side, k, :, e * capacity:(e + 1) * capacity] = jnp.where(hit, weights[:, column:column + 1], 0.0).astype(jnp.bfloat16)

    def product(entry, slot, side):
        data = jnp.concatenate([f_buf[slot, side, e] for e in range(local)], axis=0)
        total = jnp.dot(spread[entry * 2 + side, 0], data, preferred_element_type=jnp.float32)
        for k in range(1, pieces):
            total += jnp.dot(spread[entry * 2 + side, k], data, preferred_element_type=jnp.float32)
        return total

    for side in range(2):
        fetch(0, side, 0).start()
    greet(neighbour(1), neighbour(-1), neighbour(0, True))

    @pl.loop(0, n_units)
    def _(i):
        u, target = place(i)
        slot = lax.rem(i, 2)
        lane = lax.rem(i, 4)

        @pl.when(i + 1 < n_units)
        def _():
            for side in range(2):
                fetch(i + 1, side, 1 - slot).start()

        @pl.when(i == 0)
        def _():
            build(1, 0)

        @pl.when(i == 1)
        def _():
            build(2, 1)

        @pl.when(i == 8)
        def _():
            build(3, 0)

        @pl.when(i == 12)
        def _():
            build(0, 1)

        entry = 1 - lax.rem(target, 2)

        @pl.when(i >= 4)
        def _():
            swap_copy(i - 4).wait_send()
            pl.semaphore_wait(free_sem, 1)

        fetch(i, 0, slot).wait()
        other_buf[lane] = product(entry, slot, 0)
        swap_copy(i).start()
        fetch(i, 1, slot).wait()
        send_buf[i] = product(entry, slot, 1)
        swap_copy(i).wait_recv()
        send_buf[i] += swap_buf[lane]

        @pl.when(i < n_units - 4)
        def _():
            pl.semaphore_signal(free_sem, inc=1, device_id=neighbour(0, True), device_id_type=pl.DeviceIdType.MESH)

        @pl.when(i < 4)
        def _():
            ring_copy(i, u).start()

        @pl.when((i >= 8) & (i < 12))
        def _():
            ring_copy(i, u).wait_recv()
            send_buf[i] += ring_buf[u]
            ring_copy(i, u + 4).start()

    @pl.loop(0, 4)
    def _(u):
        ring_copy(0, u + 4).wait_recv()
        send_buf[u + 4] += ring_buf[u + 4]
        ring_copy(u + 4, u + 8).start()

    for u in range(4):
        swap_copy(n_units - 4 + u).wait_send()
    half = 2 * width
    loads = []
    for k in range(2):
        cols = pl.ds(k * half, half)
        loads.append(pltpu.make_async_copy(u_hbm.at[:, cols], spread.at[0, 1 + k], out_sems.at[k]))
        loads.append(pltpu.make_async_copy(h_hbm.at[:, cols], spread.at[1, k], out_sems.at[2 + k]))

    def shared_tile(t, side):
        source = (gate_hbm, up_hbm)[side]
        slot = lax.rem(t, 2)
        depth = pl.ds(pl.multiple_of(lax.rem(t, 2) * local, local), local)
        cols = pl.ds(pl.multiple_of(t // 2 * width, width), width)
        return pltpu.make_async_copy(source.at[depth, :, cols], f_buf.at[slot, side], f_sems.at[slot, side])

    def down_tile(q):
        slot = lax.rem(q, 2)
        cols = pl.ds(pl.multiple_of(q * width, width), width)
        return pltpu.make_async_copy(down_hbm.at[:, :, cols], f_buf.at[slot, 0], f_sems.at[slot, 0])

    for load in loads:
        load.start()
    for side in range(2):
        shared_tile(0, side).start()
    for load in loads:
        load.wait()

    @pl.loop(0, 4)
    def _(t):
        @pl.when(t < 3)
        def _():
            for side in range(2):
                shared_tile(t + 1, side).start()

        @pl.when(t == 3)
        def _():
            down_tile(0).start()

        k = lax.rem(t, 2)
        for side in range(2):
            shared_tile(t, side).wait()
            data = jnp.concatenate([f_buf[k, side, e] for e in range(local)], axis=0)
            part = jnp.dot(spread[0, 1 + k], data, preferred_element_type=jnp.float32)

            @pl.when(k == 0)
            def _():
                other_buf[side] = part

            @pl.when(k == 1)
            def _():
                other_buf[side] += part

        @pl.when(k == 1)
        def _():
            gate_act = other_buf[0]
            middle = gate_act * jax.nn.sigmoid(gate_act) * other_buf[1]
            spread[0, 0, :, pl.ds(pl.multiple_of(t // 2 * width, width), width)] = middle.astype(jnp.bfloat16)

    @pl.loop(0, 4)
    def _(q):
        @pl.when(q < 3)
        def _():
            down_tile(q + 1).start()

        down_tile(q).wait()
        data = jnp.concatenate([f_buf[lax.rem(q, 2), 0, e] for e in range(local)], axis=0)
        swap_buf[q] = jnp.dot(spread[0, 0], data, preferred_element_type=jnp.float32).astype(jnp.bfloat16).astype(jnp.float32)

    def put(u):
        q = quarter(u)
        inner = pl.ds(pl.multiple_of(lax.rem(q, 2) * width, width), width)
        cols = pl.ds(pl.multiple_of(q * width, width), width)
        return pltpu.make_async_copy(spread.at[3, q // 2, :, inner], out_ref.at[:, cols], out_sems.at[u])

    @pl.loop(0, 4)
    def _(u):
        q = quarter(u)
        inner = pl.ds(pl.multiple_of(lax.rem(q, 2) * width, width), width)
        ring_copy(0, u + 8).wait_recv()
        routed = send_buf[12 + u] + ring_buf[u + 8]
        spread[3, q // 2, :, inner] = (spread[1, q // 2, :, inner].astype(jnp.float32) + routed + swap_buf[q]).astype(jnp.bfloat16)
        put(u).start()

    @pl.loop(0, 4)
    def _(u):
        put(u).wait()
        ring_copy(u, u).wait_send()
        ring_copy(8 + u, u + 4).wait_send()
        ring_copy(4 + u, u + 8).wait_send()


def reduce_results(rank_t, pieces, results, residual, moe_in, gate_w, up_w, down_w):
    n_src, local, capacity, d_model = results.shape
    n_tok = rank_t.shape[1]
    width = d_model // 4
    n_pieces = pieces.shape[2] // local
    tile = (n_tok, width)
    vmem = pl.BlockSpec(memory_space=pltpu.VMEM)
    return pl.pallas_call(
        reduce_kernel,
        in_specs=[vmem, vmem] + [pl.BlockSpec(memory_space=pl.ANY)] * 6,
        out_specs=pl.BlockSpec(memory_space=pl.ANY),
        out_shape=jax.ShapeDtypeStruct((n_tok, d_model), jnp.bfloat16),
        scratch_shapes=[
            pltpu.VMEM((2, 2, local, capacity, width), jnp.bfloat16),
            pltpu.VMEM((4, n_pieces, n_tok, local * capacity), jnp.bfloat16),
            pltpu.VMEM((4,) + tile, jnp.float32),
            pltpu.VMEM((4,) + tile, jnp.float32),
            pltpu.VMEM((16,) + tile, jnp.float32),
            pltpu.VMEM((12,) + tile, jnp.float32),
            pltpu.SemaphoreType.DMA((2, 2)),
            pltpu.SemaphoreType.DMA((4,)),
            pltpu.SemaphoreType.DMA((4,)),
            pltpu.SemaphoreType.DMA((12,)),
            pltpu.SemaphoreType.DMA((12,)),
            pltpu.SemaphoreType.DMA((4,)),
            pltpu.SemaphoreType.REGULAR,
        ],
        compiler_params=pltpu.CompilerParams(vmem_limit_bytes=MAX_VMEM, collective_id=2, has_side_effects=True),
        cost_estimate=pl.CostEstimate(flops=6 * n_src * local * capacity * n_tok * d_model, bytes_accessed=4 * n_src * local * capacity * d_model, transcendentals=0),
        name="reduce_results",
    )(rank_t, pieces, results, residual, moe_in, *[w.reshape(-1, capacity, w.shape[1]) for w in (gate_w, up_w, down_w)])


def bf16_pieces(values):
    first = lax.reduce_precision(values, 8, 7)
    second = lax.reduce_precision(values - first, 8, 7)
    third = values - first - second
    return first, second, third


def local_layer(x_loc, q_shard, k_shard, v_shard, o_shard, w_router, gate_loc, up_loc, down_loc, sgate_shard, sup_shard, sdown_shard, ids_loc, group):
    n_seq, seq_len, d_model = x_loc.shape
    assert n_seq == 1 and group == 8 and q_shard.shape[2] == 128
    n_tok = n_seq * seq_len
    top_k = ids_loc.shape[-1]
    local = gate_loc.shape[0]
    n_experts = local * group
    capacity = CAP_FACTOR * n_tok * top_k // n_experts
    def gathered(shard):
        return lax.all_gather(shard.reshape(shard.shape[0], -1), 'ep', axis=0, tiled=True)

    x_flat = x_loc.reshape(n_tok, d_model)
    ids_t = ids_loc.reshape(n_tok, top_k).T
    residual, rank, ids_all = attention_layer(x_flat, ids_t, *[w.reshape(w.shape[0], -1) for w in (k_shard, v_shard, q_shard, o_shard)], group, local)
    rows, gates_all, moe_in = dispatch_tokens(residual, w_router.T, ids_t, rank, capacity)

    rank_t = rank.transpose(0, 2, 1)
    sizes = (jnp.max(rank, axis=2) + 1 + ALIGN - 1) // ALIGN * ALIGN
    ends = jnp.cumsum(sizes, axis=0)
    starts, totals = ends - sizes, ends[-1]
    rows, sgate_shard, sup_shard, sdown_shard = lax.optimization_barrier((rows, sgate_shard, sup_shard, sdown_shard))
    results = experts(sizes, starts, totals, rows, gate_loc, up_loc, down_loc)

    mine = lax.axis_index('ep') * local + jnp.arange(local)
    chosen = ids_all[:, None, :, :] == mine[None, :, None, None]
    weight = jnp.sum(jnp.where(chosen, gates_all[:, None, :, :], 0.0), axis=2)
    pieces = jnp.concatenate(bf16_pieces(weight), axis=1).transpose(0, 2, 1)

    y_out = reduce_results(rank_t, pieces, results, residual, moe_in, gathered(sgate_shard), gathered(sup_shard), gathered(sdown_shard))
    return y_out.reshape(n_seq, seq_len, d_model)


def solution(mesh):
    tok_spec = P(('dp', 'ep'), None, None)
    row_spec = P('ep', None)
    cube_spec = P('ep', None, None)
    in_specs = (tok_spec, cube_spec, cube_spec, cube_spec, row_spec, P(None, None), cube_spec, cube_spec, cube_spec, row_spec, row_spec, row_spec, tok_spec)
    return jax.shard_map(functools.partial(local_layer, group=mesh.shape['ep']), mesh=mesh, in_specs=in_specs, out_specs=tok_spec, check_vma=False)
```

```python
import functools
import jax
import jax.numpy as jnp
from jax import lax
from jax.experimental import pallas as pl
from jax.experimental.pallas import tpu as pltpu
from jax.sharding import PartitionSpec as P

EPSILON = 1e-6
CAP_FACTOR = 2
ALIGN = 16
VMEM_BYTES = 60 * 1024 * 1024
MAX_VMEM = 67043328


def rms_norm(values):
    as_f32 = values.astype(jnp.float32)
    return as_f32 * lax.rsqrt(jnp.mean(as_f32 * as_f32, axis=-1, keepdims=True) + EPSILON)


def params(**kw):
    return pltpu.CompilerParams(vmem_limit_bytes=VMEM_BYTES, **kw)


def neighbour(chips, swap=False):
    me, group = lax.axis_index('ep'), lax.axis_size('ep')
    side = lax.rem(me, 2)
    chip = lax.rem(me // 2 + chips + group // 2, group // 2)
    return {'ep': chip * 2 + (1 - side if swap else side)}


def greet(*devices):
    barrier = pltpu.get_barrier_semaphore()
    for device in devices:
        pl.semaphore_signal(barrier, inc=1, device_id=device, device_id_type=pl.DeviceIdType.MESH)
    pl.semaphore_wait(barrier, len(devices))


def remote(src, dst, send_sem, recv_sem, device):
    return pltpu.make_async_remote_copy(src_ref=src, dst_ref=dst, send_sem=send_sem, recv_sem=recv_sem, device_id=device, device_id_type=pl.DeviceIdType.MESH)


class Gather:
    def __init__(self, buf, send, recv, split=True):
        other = neighbour(0, True)
        half = buf.shape[1] // 2
        lo, hi = pl.ds(0, half), pl.ds(half, half)

        def copy(k, src, dst, device):
            return remote(src, dst, send.at[k], recv.at[k], device)

        self.own = [copy(0, buf.at[0], buf.at[1], neighbour(1)), copy(1, buf.at[0], buf.at[2], neighbour(-1))]
        self.mate = [copy(2, buf.at[0], buf.at[4], other)]
        self.near_mate = [copy(3, buf.at[1], buf.at[5], other), copy(4, buf.at[2], buf.at[6], other)]
        if split:
            self.far = [copy(5, buf.at[1, lo], buf.at[3, lo], neighbour(1)), copy(6, buf.at[2, hi], buf.at[3, hi], neighbour(-1))]
            self.far_mate = [copy(7, buf.at[3, lo], buf.at[7, lo], other), copy(8, buf.at[3, hi], buf.at[7, hi], other)]
        else:
            self.far = [copy(5, buf.at[0], buf.at[3], neighbour(2))]
            self.far_mate = [copy(7, buf.at[3], buf.at[7], other)]
        self.split = split

    def begin(self):
        for copy in self.own + self.mate + ([] if self.split else self.far):
            copy.start()

    def forward(self):
        for k in range(2):
            self.own[k].wait_recv()
            if self.split:
                self.far[k].start()
            self.near_mate[k].start()

    def forward_far(self):
        for copy, mate in zip(self.far, self.far_mate):
            copy.wait_recv()
            mate.start()

    def arrive(self, copies):
        for copy in copies:
            copy.wait_recv()

    def finish(self):
        for copy in self.own + self.mate + self.near_mate + self.far + self.far_mate:
            copy.wait_send()


def owner(r):
    step = (0, -1, 1, 2)[r % 4]
    return neighbour(step, r >= 4)['ep']


def attention_layer_kernel(x_ref, ids_ref, k_hbm, v_hbm, q_hbm, o_hbm, h_ref, rank_ref, ids_out, w_buf, n_buf, qkv, acc, ids_buf, load_sems, send, recv, ids_send, ids_recv):
    n_tok, d_model = x_ref.shape
    group, local = rank_ref.shape[:2]
    size = d_model // group
    head = 128
    width = 512
    keys, vals, queries, outs = range(4)
    gathers = [Gather(w_buf.at[w], send.at[w], recv.at[w]) for w in range(4)]
    ids_gather = Gather(ids_buf, ids_send, ids_recv, split=False)
    loads = [pltpu.make_async_copy(ref, w_buf.at[w, 0], load_sems.at[w]) for w, ref in enumerate((k_hbm, v_hbm, q_hbm, o_hbm))]
    ids_load = pltpu.make_async_copy(ids_ref, ids_buf.at[0], load_sems.at[4])
    ids_load.start()
    for load in loads:
        load.start()
    greet(neighbour(1), neighbour(-1), neighbour(2), neighbour(0, True))
    ids_load.wait()
    ids_gather.begin()
    for w in (keys, vals):
        loads[w].wait()
        gathers[w].begin()

    @pl.loop(0, n_tok // 128)
    def _(i):
        rows = pl.ds(pl.multiple_of(i * 128, 128), 128)
        normed = rms_norm(x_ref[rows, :]).astype(jnp.bfloat16)
        qkv[0, rows, :] = normed
        for r in range(group):
            n_buf[rows, r * size:(r + 1) * size] = qkv[0, rows, pl.ds(pl.multiple_of(owner(r) * size, size), size)]

    ids_gather.arrive(ids_gather.own + ids_gather.mate)
    for copy in ids_gather.near_mate:
        copy.start()
    ids_gather.forward_far()
    ids_gather.arrive(ids_gather.near_mate + ids_gather.far_mate)
    first = lax.axis_index('ep') * local
    before = (lax.broadcasted_iota(jnp.int32, (n_tok, n_tok), 0) < lax.broadcasted_iota(jnp.int32, (n_tok, n_tok), 1)).astype(jnp.float32).astype(jnp.bfloat16)
    for r in range(group):
        member = jnp.concatenate([jnp.max((ids_buf[r] == first + e).astype(jnp.float32), axis=0, keepdims=True) for e in range(local)], axis=0)
        rank = jnp.dot(member.astype(jnp.bfloat16), before, preferred_element_type=jnp.float32)
        rank_ref[r] = jnp.where(member > 0.5, rank, -1.0).astype(jnp.int32)

    def project(w, store):
        @pl.loop(0, d_model // width)
        def _(c):
            cols = pl.ds(pl.multiple_of(c * width, width), width)
            weight = jnp.concatenate([w_buf[w, r, :, cols] for r in range(group)], axis=0)
            store(cols, jnp.dot(n_buf[...], weight, preferred_element_type=jnp.float32).astype(jnp.bfloat16))

    def keep(w):
        def store(cols, values):
            qkv[w, :, cols] = values
        return store

    def complete(w):
        gathers[w].forward_far()
        gathers[w].arrive(gathers[w].mate + gathers[w].near_mate + gathers[w].far_mate)

    def attend(lo, hi):
        for r in range(lo, hi):
            start = owner(r) * size

            @pl.loop(0, size // head)
            def _(k):
                cols = pl.ds(pl.multiple_of(start + k * head, head), head)
                parts = 2
                step = n_tok // parts
                for part in range(parts):
                    top, end = part * step, (part + 1) * step
                    scores = lax.dot_general(qkv[queries, top:end, cols], qkv[keys, :end, cols], (((1,), (1,)), ((), ())), preferred_element_type=jnp.float32) * (head ** -0.5)
                    row = top + lax.broadcasted_iota(jnp.int32, scores.shape, 0)
                    col = lax.broadcasted_iota(jnp.int32, scores.shape, 1)
                    scores = jnp.where(row >= col, scores, -1e30)
                    weights = jnp.exp(scores - jnp.max(scores, axis=-1, keepdims=True))
                    probs = (weights / jnp.sum(weights, axis=-1, keepdims=True)).astype(jnp.bfloat16)
                    n_buf[top:end, pl.ds(pl.multiple_of(r * size + k * head, head), head)] = jnp.dot(probs, qkv[vals, :end, cols], preferred_element_type=jnp.float32).astype(jnp.bfloat16)

    gathers[keys].forward()
    loads[queries].wait()
    gathers[queries].begin()
    gathers[vals].forward()
    complete(keys)
    project(keys, keep(keys))
    gathers[queries].forward()
    loads[outs].wait()
    gathers[outs].begin()
    complete(vals)
    project(vals, keep(vals))
    complete(queries)
    project(queries, keep(queries))
    attend(0, group // 2)
    gathers[outs].forward()
    attend(group // 2, group)
    gathers[outs].arrive(gathers[outs].mate + gathers[outs].near_mate)
    side = group // 2
    spans = [(r0 * size, (r0 + side - 1) * size) for r0 in (0, side)]

    @pl.loop(0, d_model // width)
    def _(c):
        cols = pl.ds(pl.multiple_of(c * width, width), width)
        weights = [jnp.concatenate([w_buf[outs, r, :, cols] for r in range(r0, r0 + side - 1)], axis=0) for r0 in (0, side)]
        parts = [jnp.dot(n_buf[:, lo:hi], weight, preferred_element_type=jnp.float32) for (lo, hi), weight in zip(spans, weights)]
        acc[:, cols] = parts[0] + parts[1]

    gathers[outs].forward_far()
    gathers[outs].arrive(gathers[outs].far_mate)

    @pl.loop(0, d_model // width)
    def _(c):
        cols = pl.ds(pl.multiple_of(c * width, width), width)
        parts = [jnp.dot(n_buf[:, hi:hi + size], w_buf[outs, hi // size, :, cols], preferred_element_type=jnp.float32) for lo, hi in spans]
        attn = (acc[:, cols] + parts[0] + parts[1]).astype(jnp.bfloat16)
        h_ref[:, cols] = (x_ref[:, cols].astype(jnp.float32) + attn.astype(jnp.float32)).astype(jnp.bfloat16)

    for r in range(group):
        ids_out[r] = ids_buf[r]
    for gather in gathers + [ids_gather]:
        gather.finish()


def attention_layer(x, ids_t, k_shard, v_shard, q_shard, o_shard, group, local):
    n_tok, d_model = x.shape
    top_k = ids_t.shape[0]
    vmem = pl.BlockSpec(memory_space=pltpu.VMEM)
    anywhere = pl.BlockSpec(memory_space=pl.ANY)
    return pl.pallas_call(
        attention_layer_kernel,
        in_specs=[vmem] + [anywhere] * 5,
        out_specs=[vmem] * 3,
        out_shape=[jax.ShapeDtypeStruct(x.shape, jnp.bfloat16), jax.ShapeDtypeStruct((group, local, n_tok), jnp.int32), jax.ShapeDtypeStruct((group, top_k, n_tok), jnp.int32)],
        scratch_shapes=[
            pltpu.VMEM((4, group) + k_shard.shape, jnp.bfloat16),
            pltpu.VMEM(x.shape, jnp.bfloat16),
            pltpu.VMEM((3,) + x.shape, jnp.bfloat16),
            pltpu.VMEM(x.shape, jnp.float32),
            pltpu.VMEM((group, top_k, n_tok), jnp.int32),
            pltpu.SemaphoreType.DMA((5,)),
            pltpu.SemaphoreType.DMA((4, 9)),
            pltpu.SemaphoreType.DMA((4, 9)),
            pltpu.SemaphoreType.DMA((9,)),
            pltpu.SemaphoreType.DMA((9,)),
        ],
        compiler_params=pltpu.CompilerParams(vmem_limit_bytes=MAX_VMEM, collective_id=0, has_side_effects=True),
        cost_estimate=pl.CostEstimate(flops=9 * n_tok * d_model * d_model, bytes_accessed=8 * d_model * d_model // group, transcendentals=0),
        name="attention_layer",
    )(x, ids_t, k_shard, v_shard, q_shard, o_shard)


def dispatch_kernel(h_ref, wr_ref, ids_ref, rank_ref, x_hbm, gates_ref, u_hbm, u_buf, pick, stage, g_buf, out_sems, send, recv, g_send, g_recv):
    n_tok, d_model = h_ref.shape
    group, local = rank_ref.shape[:2]
    capacity = x_hbm.shape[2]
    n_experts = wr_ref.shape[0]
    top_k = ids_ref.shape[0]
    width = stage.shape[3]
    n_cols = d_model // width
    tokens = Gather(u_buf, send, recv)
    gates = Gather(g_buf, g_send, g_recv, split=False)

    @pl.loop(0, n_tok // 128)
    def _(i):
        rows = pl.ds(pl.multiple_of(i * 128, 128), 128)
        u_buf[0, rows, :] = rms_norm(h_ref[rows, :]).astype(jnp.bfloat16)

    greet(neighbour(1), neighbour(-1), neighbour(2), neighbour(0, True))
    tokens.begin()
    keep = pltpu.make_async_copy(u_buf.at[0], u_hbm, out_sems.at[2])
    keep.start()

    for i in range(n_tok // 128):
        rows = slice(i * 128, (i + 1) * 128)
        logits = lax.dot_general(wr_ref[...], rms_norm(h_ref[rows, :]), (((1,), (1,)), ((), ())), precision=lax.Precision.HIGHEST, preferred_element_type=jnp.float32)
        experts_iota = lax.broadcasted_iota(jnp.int32, (n_experts, 128), 0)
        chosen = jnp.concatenate([jnp.sum(jnp.where(experts_iota == ids_ref[j:j + 1, rows], logits, 0.0), axis=0, keepdims=True) for j in range(top_k)], axis=0)
        weights = jnp.exp(chosen - jnp.max(chosen, axis=0, keepdims=True))
        g_buf[0, :, rows] = weights / jnp.sum(weights, axis=0, keepdims=True)
    gates.begin()

    def put(r, c, slot):
        cols = pl.ds(pl.multiple_of(c * width, width), width)
        return pltpu.make_async_copy(stage.at[slot], x_hbm.at[r, :, :, cols], out_sems.at[slot])

    def dispatch(r, before):
        slots = lax.broadcasted_iota(jnp.int32, (capacity, n_tok), 0)
        for e in range(local):
            pick[e * capacity:(e + 1) * capacity, :] = (rank_ref[r, e:e + 1, :] == slots).astype(jnp.float32).astype(jnp.bfloat16)

        @pl.loop(0, n_cols)
        def _(c):
            slot = lax.rem(c, 2)
            cols = pl.ds(pl.multiple_of(c * width, width), width)
            if before is None:
                @pl.when(c >= 2)
                def _():
                    put(r, c - 2, slot).wait()
            else:
                @pl.when(c >= 2)
                def _():
                    put(r, c - 2, slot).wait()

                @pl.when(c < 2)
                def _():
                    put(before, n_cols - 2 + c, slot).wait()
            rows = jnp.dot(pick[...], u_buf[r, :, cols], preferred_element_type=jnp.float32).astype(jnp.bfloat16)
            for e in range(local):
                stage[slot, e] = rows[e * capacity:(e + 1) * capacity, :]
            put(r, c, slot).start()

    dispatch(0, None)
    tokens.arrive(tokens.mate)
    dispatch(4, 0)
    tokens.forward()
    dispatch(1, 4)
    dispatch(2, 1)
    gates.arrive(gates.own + gates.mate)
    for copy in gates.near_mate:
        copy.start()
    gates.forward_far()
    tokens.arrive(tokens.near_mate)
    dispatch(5, 2)
    dispatch(6, 5)
    tokens.forward_far()
    gates.arrive(gates.near_mate + gates.far_mate)
    for r in range(group):
        gates_ref[r] = g_buf[r]
    dispatch(3, 6)
    tokens.arrive(tokens.far_mate)
    dispatch(7, 3)
    for c in range(n_cols - 2, n_cols):
        put(7, c, c % 2).wait()
    keep.wait()
    tokens.finish()
    gates.finish()


def dispatch_tokens(h, router_t, ids_t, rank, capacity):
    n_tok, d_model = h.shape
    group, local = rank.shape[:2]
    top_k = ids_t.shape[0]
    width = 512
    vmem = pl.BlockSpec(memory_space=pltpu.VMEM)
    return pl.pallas_call(
        dispatch_kernel,
        in_specs=[vmem] * 4,
        out_specs=[pl.BlockSpec(memory_space=pl.ANY), vmem, pl.BlockSpec(memory_space=pl.ANY)],
        out_shape=[jax.ShapeDtypeStruct((group, local, capacity, d_model), jnp.bfloat16), jax.ShapeDtypeStruct((group, top_k, n_tok), jnp.float32), jax.ShapeDtypeStruct(h.shape, jnp.bfloat16)],
        scratch_shapes=[
            pltpu.VMEM((group, n_tok, d_model), jnp.bfloat16),
            pltpu.VMEM((local * capacity, n_tok), jnp.bfloat16),
            pltpu.VMEM((2, local, capacity, width), jnp.bfloat16),
            pltpu.VMEM((group, top_k, n_tok), jnp.float32),
            pltpu.SemaphoreType.DMA((3,)),
            pltpu.SemaphoreType.DMA((9,)),
            pltpu.SemaphoreType.DMA((9,)),
            pltpu.SemaphoreType.DMA((9,)),
            pltpu.SemaphoreType.DMA((9,)),
        ],
        compiler_params=pltpu.CompilerParams(vmem_limit_bytes=MAX_VMEM, collective_id=1, has_side_effects=True),
        cost_estimate=pl.CostEstimate(flops=2 * group * local * capacity * n_tok * d_model, bytes_accessed=2 * group * local * capacity * d_model, transcendentals=0),
        name="dispatch_tokens",
    )(h, router_t, ids_t, rank)


def expert_kernel(size_ref, start_ref, total_ref, x_ref, gate_ref, up_ref, down_ref, f_ref, x_buf, f_buf, in_sems, out_sems, *, chunk):
    n_src, _, capacity, d_model = x_ref.shape
    e, local = pl.program_id(0), pl.num_programs(0)
    slot = lax.rem(e, 2)
    zeros = jnp.zeros((capacity, d_model), jnp.bfloat16)

    def fetch(r, expert, where):
        size = pl.multiple_of(size_ref[r, expert], ALIGN)
        start = pl.multiple_of(start_ref[r, expert], ALIGN)
        return pltpu.make_async_copy(x_ref.at[r, expert, pl.ds(0, size), :], x_buf.at[where, pl.ds(start, size), :], in_sems.at[where, r])

    def put(r, expert, where):
        start = pl.multiple_of(start_ref[r, expert], ALIGN)
        return pltpu.make_async_copy(f_buf.at[where, pl.ds(start, capacity), :], f_ref.at[r, expert], out_sems.at[where, r])

    @pl.when(e == 0)
    def _():
        for r in range(n_src):
            fetch(r, 0, 0).start()

    @pl.when(e + 1 < local)
    def _():
        for r in range(n_src):
            fetch(r, e + 1, 1 - slot).start()

    for r in range(n_src):
        fetch(r, e, slot).wait()

    @pl.when(e >= 2)
    def _():
        for r in range(n_src):
            put(r, e - 2, slot).wait()

    total = total_ref[e]
    x_buf[slot, pl.ds(pl.multiple_of(total, ALIGN), capacity), :] = zeros
    chunks = (total + chunk - 1) // chunk

    def run(start, size):
        rows = pl.ds(pl.multiple_of(start, chunk), size)
        x = x_buf[slot, rows, :]
        gate_act = jnp.dot(x, gate_ref[0], preferred_element_type=jnp.float32)
        up_act = jnp.dot(x, up_ref[0], preferred_element_type=jnp.float32)
        middle = (gate_act * jax.nn.sigmoid(gate_act) * up_act).astype(jnp.bfloat16)
        f_buf[slot, rows, :] = jnp.dot(middle, down_ref[0], preferred_element_type=jnp.float32).astype(jnp.bfloat16)

    @pl.loop(0, chunks // 2)
    def _(i):
        run(i * 2 * chunk, 2 * chunk)

    @pl.when(lax.rem(chunks, 2) == 1)
    def _():
        run((chunks - 1) * chunk, chunk)

    f_buf[slot, pl.ds(pl.multiple_of(chunks * chunk, chunk), capacity), :] = zeros
    for r in range(n_src):
        put(r, e, slot).start()

    @pl.when(e == local - 1)
    def _():
        @pl.when(e >= 1)
        def _():
            for r in range(n_src):
                put(r, e - 1, 1 - slot).wait()
        for r in range(n_src):
            put(r, e, slot).wait()


def experts(sizes, starts, totals, rows, gate_w, up_w, down_w):
    n_src, local, capacity, d_model = rows.shape
    width = gate_w.shape[2]
    chunk = capacity
    n_rows = n_src * capacity + 2 * capacity
    anywhere = pl.BlockSpec(memory_space=pl.ANY)
    return pl.pallas_call(
        functools.partial(expert_kernel, chunk=chunk),
        grid_spec=pltpu.PrefetchScalarGridSpec(
            num_scalar_prefetch=3,
            grid=(local,),
            in_specs=[anywhere] + [
                pl.BlockSpec((1, d_model, width), lambda e, *_: (e, 0, 0)),
                pl.BlockSpec((1, d_model, width), lambda e, *_: (e, 0, 0)),
                pl.BlockSpec((1, width, d_model), lambda e, *_: (e, 0, 0)),
            ],
            out_specs=anywhere,
            scratch_shapes=[
                pltpu.VMEM((2, n_rows, d_model), jnp.bfloat16),
                pltpu.VMEM((2, n_rows, d_model), jnp.bfloat16),
                pltpu.SemaphoreType.DMA((2, n_src)),
                pltpu.SemaphoreType.DMA((2, n_src)),
            ],
        ),
        out_shape=jax.ShapeDtypeStruct(rows.shape, jnp.bfloat16),
        compiler_params=params(),
        cost_estimate=pl.CostEstimate(flops=4 * local * n_src * capacity * d_model * width, bytes_accessed=6 * local * d_model * width, transcendentals=0),
        name="experts",
    )(sizes, starts, totals, rows, gate_w, up_w, down_w)


def reduce_kernel(rank_ref, ids_ref, gates_ref, f_ref, h_hbm, u_hbm, gate_hbm, up_hbm, down_hbm, out_ref, f_buf, spread, other_buf, swap_buf, send_buf, ring_buf, f_sems, swap_send, swap_recv, ring_send, ring_recv, out_sems, free_sem):
    n_src, local, n_tok = rank_ref.shape
    capacity = f_ref.shape[2]
    top_k = ids_ref.shape[1]
    pieces = spread.shape[1]
    chips = n_src // 2
    width = out_ref.shape[1] // 4
    n_units = 16

    def quarter(u):
        return 2 * lax.rem(u, 2) + u // 2

    def place(i):
        u = lax.rem(i, 4)
        odd = lax.rem(u, 2)
        target = jnp.where(i < 4, 1 + odd, jnp.where(i < 8, 2 - odd, jnp.where(i < 12, 3, 0)))
        return u, target

    def fetch(i, side, slot):
        u, target = place(i)
        cols = pl.ds(pl.multiple_of(quarter(u) * width, width), width)
        return pltpu.make_async_copy(f_ref.at[target + chips * (1 - side), :, :, cols], f_buf.at[slot, side], f_sems.at[slot, side])

    def swap_copy(i):
        s = lax.rem(i, 4)
        return remote(other_buf.at[s], swap_buf.at[s], swap_send.at[s], swap_recv.at[s], neighbour(0, True))

    def ring_copy(source, slot):
        return remote(send_buf.at[source], ring_buf.at[slot], ring_send.at[slot], ring_recv.at[slot], neighbour(1 - 2 * lax.rem(slot, 2)))

    def build(target, entry):
        @pl.loop(0, 2)
        def _(side):
            r = target + chips * (1 - side)
            first = lax.axis_index('ep') * local
            ids = ids_ref[r]
            gates = gates_ref[r]
            rest = jnp.concatenate([jnp.sum(jnp.where(ids == first + e, gates, 0.0), axis=0, keepdims=True) for e in range(local)], axis=0)
            table = [rank_ref[r].astype(jnp.float32)]
            for _ in range(pieces):
                table.append(rest.astype(jnp.bfloat16).astype(jnp.float32))
                rest = rest - table[-1]
            table = jnp.concatenate(table, axis=0).T
            rank = table[:, :local].astype(jnp.int32)
            weights = table[:, local:]
            slots = lax.broadcasted_iota(jnp.int32, (n_tok, capacity), 1)
            for e in range(local):
                hit = rank[:, e:e + 1] == slots
                for k in range(pieces):
                    column = k * local + e
                    spread[entry * 2 + side, k, :, e * capacity:(e + 1) * capacity] = jnp.where(hit, weights[:, column:column + 1], 0.0).astype(jnp.bfloat16)

    def product(entry, slot, side):
        data = jnp.concatenate([f_buf[slot, side, e] for e in range(local)], axis=0)
        total = jnp.dot(spread[entry * 2 + side, 0], data, preferred_element_type=jnp.float32)
        for k in range(1, pieces):
            total += jnp.dot(spread[entry * 2 + side, k], data, preferred_element_type=jnp.float32)
        return total

    for side in range(2):
        fetch(0, side, 0).start()
    greet(neighbour(1), neighbour(-1), neighbour(0, True))

    @pl.loop(0, n_units)
    def _(i):
        u, target = place(i)
        slot = lax.rem(i, 2)
        lane = lax.rem(i, 4)

        @pl.when(i + 1 < n_units)
        def _():
            for side in range(2):
                fetch(i + 1, side, 1 - slot).start()

        @pl.when(i == 0)
        def _():
            build(1, 0)

        @pl.when(i == 1)
        def _():
            build(2, 1)

        @pl.when(i == 8)
        def _():
            build(3, 0)

        @pl.when(i == 12)
        def _():
            build(0, 1)

        entry = 1 - lax.rem(target, 2)

        @pl.when(i >= 4)
        def _():
            swap_copy(i - 4).wait_send()
            pl.semaphore_wait(free_sem, 1)

        fetch(i, 0, slot).wait()
        other_buf[lane] = product(entry, slot, 0)
        swap_copy(i).start()
        fetch(i, 1, slot).wait()
        send_buf[i] = product(entry, slot, 1)
        swap_copy(i).wait_recv()
        send_buf[i] += swap_buf[lane]

        @pl.when(i < n_units - 4)
        def _():
            pl.semaphore_signal(free_sem, inc=1, device_id=neighbour(0, True), device_id_type=pl.DeviceIdType.MESH)

        @pl.when(i < 4)
        def _():
            ring_copy(i, u).start()

        @pl.when((i >= 8) & (i < 12))
        def _():
            ring_copy(i, u).wait_recv()
            send_buf[i] += ring_buf[u]
            ring_copy(i, u + 4).start()

    @pl.loop(0, 4)
    def _(u):
        ring_copy(0, u + 4).wait_recv()
        send_buf[u + 4] += ring_buf[u + 4]
        ring_copy(u + 4, u + 8).start()

    for u in range(4):
        swap_copy(n_units - 4 + u).wait_send()
    half = 2 * width
    loads = []
    for k in range(2):
        cols = pl.ds(k * half, half)
        loads.append(pltpu.make_async_copy(u_hbm.at[:, cols], spread.at[0, 1 + k], out_sems.at[k]))
        loads.append(pltpu.make_async_copy(h_hbm.at[:, cols], spread.at[1, k], out_sems.at[2 + k]))

    def shared_tile(t, side):
        source = (gate_hbm, up_hbm)[side]
        slot = lax.rem(t, 2)
        depth = pl.ds(pl.multiple_of(lax.rem(t, 2) * local, local), local)
        cols = pl.ds(pl.multiple_of(t // 2 * width, width), width)
        return pltpu.make_async_copy(source.at[depth, :, cols], f_buf.at[slot, side], f_sems.at[slot, side])

    def down_tile(q):
        slot = lax.rem(q, 2)
        cols = pl.ds(pl.multiple_of(q * width, width), width)
        return pltpu.make_async_copy(down_hbm.at[:, :, cols], f_buf.at[slot, 0], f_sems.at[slot, 0])

    for load in loads:
        load.start()
    for side in range(2):
        shared_tile(0, side).start()
    for load in loads:
        load.wait()

    @pl.loop(0, 4)
    def _(t):
        @pl.when(t < 3)
        def _():
            for side in range(2):
                shared_tile(t + 1, side).start()

        @pl.when(t == 3)
        def _():
            down_tile(0).start()

        k = lax.rem(t, 2)
        for side in range(2):
            shared_tile(t, side).wait()
            data = jnp.concatenate([f_buf[k, side, e] for e in range(local)], axis=0)
            part = jnp.dot(spread[0, 1 + k], data, preferred_element_type=jnp.float32)

            @pl.when(k == 0)
            def _():
                other_buf[side] = part

            @pl.when(k == 1)
            def _():
                other_buf[side] += part

        @pl.when(k == 1)
        def _():
            gate_act = other_buf[0]
            middle = gate_act * jax.nn.sigmoid(gate_act) * other_buf[1]
            spread[0, 0, :, pl.ds(pl.multiple_of(t // 2 * width, width), width)] = middle.astype(jnp.bfloat16)

    @pl.loop(0, 4)
    def _(q):
        @pl.when(q < 3)
        def _():
            down_tile(q + 1).start()

        down_tile(q).wait()
        data = jnp.concatenate([f_buf[lax.rem(q, 2), 0, e] for e in range(local)], axis=0)
        swap_buf[q] = jnp.dot(spread[0, 0], data, preferred_element_type=jnp.float32).astype(jnp.bfloat16).astype(jnp.float32)

    def put(u):
        q = quarter(u)
        inner = pl.ds(pl.multiple_of(lax.rem(q, 2) * width, width), width)
        cols = pl.ds(pl.multiple_of(q * width, width), width)
        return pltpu.make_async_copy(spread.at[3, q // 2, :, inner], out_ref.at[:, cols], out_sems.at[u])

    @pl.loop(0, 4)
    def _(u):
        q = quarter(u)
        inner = pl.ds(pl.multiple_of(lax.rem(q, 2) * width, width), width)
        ring_copy(0, u + 8).wait_recv()
        routed = send_buf[12 + u] + ring_buf[u + 8]
        spread[3, q // 2, :, inner] = (spread[1, q // 2, :, inner].astype(jnp.float32) + routed + swap_buf[q]).astype(jnp.bfloat16)
        put(u).start()

    @pl.loop(0, 4)
    def _(u):
        put(u).wait()
        ring_copy(u, u).wait_send()
        ring_copy(8 + u, u + 4).wait_send()
        ring_copy(4 + u, u + 8).wait_send()


def reduce_results(rank, ids, gates, results, residual, moe_in, gate_w, up_w, down_w):
    n_src, local, capacity, d_model = results.shape
    n_tok = rank.shape[2]
    width = d_model // 4
    n_pieces = 3
    tile = (n_tok, width)
    vmem = pl.BlockSpec(memory_space=pltpu.VMEM)
    return pl.pallas_call(
        reduce_kernel,
        in_specs=[vmem] * 3 + [pl.BlockSpec(memory_space=pl.ANY)] * 6,
        out_specs=pl.BlockSpec(memory_space=pl.ANY),
        out_shape=jax.ShapeDtypeStruct((n_tok, d_model), jnp.bfloat16),
        scratch_shapes=[
            pltpu.VMEM((2, 2, local, capacity, width), jnp.bfloat16),
            pltpu.VMEM((4, n_pieces, n_tok, local * capacity), jnp.bfloat16),
            pltpu.VMEM((4,) + tile, jnp.float32),
            pltpu.VMEM((4,) + tile, jnp.float32),
            pltpu.VMEM((16,) + tile, jnp.float32),
            pltpu.VMEM((12,) + tile, jnp.float32),
            pltpu.SemaphoreType.DMA((2, 2)),
            pltpu.SemaphoreType.DMA((4,)),
            pltpu.SemaphoreType.DMA((4,)),
            pltpu.SemaphoreType.DMA((12,)),
            pltpu.SemaphoreType.DMA((12,)),
            pltpu.SemaphoreType.DMA((4,)),
            pltpu.SemaphoreType.REGULAR,
        ],
        compiler_params=pltpu.CompilerParams(vmem_limit_bytes=MAX_VMEM, collective_id=2, has_side_effects=True),
        cost_estimate=pl.CostEstimate(flops=6 * n_src * local * capacity * n_tok * d_model, bytes_accessed=4 * n_src * local * capacity * d_model, transcendentals=0),
        name="reduce_results",
    )(rank, ids, gates, results, residual, moe_in, *[w.reshape(-1, capacity, w.shape[1]) for w in (gate_w, up_w, down_w)])


def local_layer(x_loc, q_shard, k_shard, v_shard, o_shard, w_router, gate_loc, up_loc, down_loc, sgate_shard, sup_shard, sdown_shard, ids_loc, group):
    n_seq, seq_len, d_model = x_loc.shape
    assert n_seq == 1 and group == 8 and q_shard.shape[2] == 128
    n_tok = n_seq * seq_len
    top_k = ids_loc.shape[-1]
    local = gate_loc.shape[0]
    n_experts = local * group
    capacity = CAP_FACTOR * n_tok * top_k // n_experts
    def gathered(shard):
        return lax.all_gather(shard.reshape(shard.shape[0], -1), 'ep', axis=0, tiled=True)

    x_flat = x_loc.reshape(n_tok, d_model)
    ids_t = ids_loc.reshape(n_tok, top_k).T
    residual, rank, ids_all = attention_layer(x_flat, ids_t, *[w.reshape(w.shape[0], -1) for w in (k_shard, v_shard, q_shard, o_shard)], group, local)
    rows, gates_all, moe_in = dispatch_tokens(residual, w_router.T, ids_t, rank, capacity)

    sizes = (jnp.max(rank, axis=2) + 1 + ALIGN - 1) // ALIGN * ALIGN
    ends = jnp.cumsum(sizes, axis=0)
    starts, totals = ends - sizes, ends[-1]
    rows, sgate_shard, sup_shard, sdown_shard = lax.optimization_barrier((rows, sgate_shard, sup_shard, sdown_shard))
    results = experts(sizes, starts, totals, rows, gate_loc, up_loc, down_loc)

    y_out = reduce_results(rank, ids_all, gates_all, results, residual, moe_in, gathered(sgate_shard), gathered(sup_shard), gathered(sdown_shard))
    return y_out.reshape(n_seq, seq_len, d_model)


def solution(mesh):
    tok_spec = P(('dp', 'ep'), None, None)
    row_spec = P('ep', None)
    cube_spec = P('ep', None, None)
    in_specs = (tok_spec, cube_spec, cube_spec, cube_spec, row_spec, P(None, None), cube_spec, cube_spec, cube_spec, row_spec, row_spec, row_spec, tok_spec)
    return jax.shard_map(functools.partial(local_layer, group=mesh.shape['ep']), mesh=mesh, in_specs=in_specs, out_specs=tok_spec, check_vma=False)
```

```python
import functools
import jax
import jax.numpy as jnp
from jax import lax
from jax.experimental import pallas as pl
from jax.experimental.pallas import tpu as pltpu
from jax.sharding import PartitionSpec as P

EPSILON = 1e-6
CAP_FACTOR = 2
ALIGN = 16
VMEM_BYTES = 60 * 1024 * 1024
MAX_VMEM = 67043328


def rms_norm(values):
    as_f32 = values.astype(jnp.float32)
    return as_f32 * lax.rsqrt(jnp.mean(as_f32 * as_f32, axis=-1, keepdims=True) + EPSILON)


def params(**kw):
    return pltpu.CompilerParams(vmem_limit_bytes=VMEM_BYTES, **kw)


def neighbour(chips, swap=False):
    me, group = lax.axis_index('ep'), lax.axis_size('ep')
    side = lax.rem(me, 2)
    chip = lax.rem(me // 2 + chips + group // 2, group // 2)
    return {'ep': chip * 2 + (1 - side if swap else side)}


def greet(*devices):
    barrier = pltpu.get_barrier_semaphore()
    for device in devices:
        pl.semaphore_signal(barrier, inc=1, device_id=device, device_id_type=pl.DeviceIdType.MESH)
    pl.semaphore_wait(barrier, len(devices))


def remote(src, dst, send_sem, recv_sem, device):
    return pltpu.make_async_remote_copy(src_ref=src, dst_ref=dst, send_sem=send_sem, recv_sem=recv_sem, device_id=device, device_id_type=pl.DeviceIdType.MESH)


class Gather:
    def __init__(self, buf, send, recv, split=True):
        other = neighbour(0, True)
        half = buf.shape[1] // 2
        lo, hi = pl.ds(0, half), pl.ds(half, half)

        def copy(k, src, dst, device):
            return remote(src, dst, send.at[k], recv.at[k], device)

        self.own = [copy(0, buf.at[0], buf.at[1], neighbour(1)), copy(1, buf.at[0], buf.at[2], neighbour(-1))]
        self.mate = [copy(2, buf.at[0], buf.at[4], other)]
        self.near_mate = [copy(3, buf.at[1], buf.at[5], other), copy(4, buf.at[2], buf.at[6], other)]
        if split:
            self.far = [copy(5, buf.at[1, lo], buf.at[3, lo], neighbour(1)), copy(6, buf.at[2, hi], buf.at[3, hi], neighbour(-1))]
            self.far_mate = [copy(7, buf.at[3, lo], buf.at[7, lo], other), copy(8, buf.at[3, hi], buf.at[7, hi], other)]
        else:
            self.far = [copy(5, buf.at[0], buf.at[3], neighbour(2))]
            self.far_mate = [copy(7, buf.at[3], buf.at[7], other)]
        self.split = split

    def begin(self):
        for copy in self.own + self.mate + ([] if self.split else self.far):
            copy.start()

    def forward(self):
        for k in range(2):
            self.own[k].wait_recv()
            if self.split:
                self.far[k].start()
            self.near_mate[k].start()

    def forward_far(self):
        for copy, mate in zip(self.far, self.far_mate):
            copy.wait_recv()
            mate.start()

    def arrive(self, copies):
        for copy in copies:
            copy.wait_recv()

    def finish(self):
        for copy in self.own + self.mate + self.near_mate + self.far + self.far_mate:
            copy.wait_send()


def owner(r):
    step = (0, -1, 1, 2)[r % 4]
    return neighbour(step, r >= 4)['ep']


def attention_layer_kernel(x_ref, ids_ref, k_hbm, v_hbm, q_hbm, o_hbm, h_ref, rank_ref, ids_out, w_buf, n_buf, qkv, acc, ids_buf, load_sems, send, recv, ids_send, ids_recv):
    n_tok, d_model = x_ref.shape
    group, local = rank_ref.shape[:2]
    size = d_model // group
    head = 128
    width = 512
    keys, vals, queries, outs = range(4)
    gathers = [Gather(w_buf.at[w], send.at[w], recv.at[w]) for w in range(4)]
    ids_gather = Gather(ids_buf, ids_send, ids_recv, split=False)
    loads = [pltpu.make_async_copy(ref, w_buf.at[w, 0], load_sems.at[w]) for w, ref in enumerate((k_hbm, v_hbm, q_hbm, o_hbm))]
    ids_load = pltpu.make_async_copy(ids_ref, ids_buf.at[0], load_sems.at[4])
    ids_load.start()
    for load in loads:
        load.start()
    greet(neighbour(1), neighbour(-1), neighbour(2), neighbour(0, True))
    ids_load.wait()
    ids_gather.begin()
    for w in (keys, vals):
        loads[w].wait()
        gathers[w].begin()

    @pl.loop(0, n_tok // 128)
    def _(i):
        rows = pl.ds(pl.multiple_of(i * 128, 128), 128)
        normed = rms_norm(x_ref[rows, :]).astype(jnp.bfloat16)
        qkv[0, rows, :] = normed
        for r in range(group):
            n_buf[rows, r * size:(r + 1) * size] = qkv[0, rows, pl.ds(pl.multiple_of(owner(r) * size, size), size)]

    ids_gather.arrive(ids_gather.own + ids_gather.mate)
    for copy in ids_gather.near_mate:
        copy.start()
    ids_gather.forward_far()
    ids_gather.arrive(ids_gather.near_mate + ids_gather.far_mate)
    first = lax.axis_index('ep') * local
    before = (lax.broadcasted_iota(jnp.int32, (n_tok, n_tok), 0) < lax.broadcasted_iota(jnp.int32, (n_tok, n_tok), 1)).astype(jnp.float32).astype(jnp.bfloat16)
    for r in range(group):
        member = jnp.concatenate([jnp.max((ids_buf[r] == first + e).astype(jnp.float32), axis=0, keepdims=True) for e in range(local)], axis=0)
        rank = jnp.dot(member.astype(jnp.bfloat16), before, preferred_element_type=jnp.float32)
        rank_ref[r] = jnp.where(member > 0.5, rank, -1.0).astype(jnp.int32)

    def project(w, store):
        @pl.loop(0, d_model // width)
        def _(c):
            cols = pl.ds(pl.multiple_of(c * width, width), width)
            weight = jnp.concatenate([w_buf[w, r, :, cols] for r in range(group)], axis=0)
            store(cols, jnp.dot(n_buf[...], weight, preferred_element_type=jnp.float32).astype(jnp.bfloat16))

    def keep(w):
        def store(cols, values):
            qkv[w, :, cols] = values
        return store

    def complete(w):
        gathers[w].forward_far()
        gathers[w].arrive(gathers[w].mate + gathers[w].near_mate + gathers[w].far_mate)

    def attend(lo, hi):
        for r in range(lo, hi):
            start = owner(r) * size

            @pl.loop(0, size // head)
            def _(k):
                cols = pl.ds(pl.multiple_of(start + k * head, head), head)
                parts = 2
                step = n_tok // parts
                for part in range(parts):
                    top, end = part * step, (part + 1) * step
                    scores = lax.dot_general(qkv[queries, top:end, cols], qkv[keys, :end, cols], (((1,), (1,)), ((), ())), preferred_element_type=jnp.float32) * (head ** -0.5)
                    row = top + lax.broadcasted_iota(jnp.int32, scores.shape, 0)
                    col = lax.broadcasted_iota(jnp.int32, scores.shape, 1)
                    scores = jnp.where(row >= col, scores, -1e30)
                    weights = jnp.exp(scores - jnp.max(scores, axis=-1, keepdims=True))
                    probs = (weights / jnp.sum(weights, axis=-1, keepdims=True)).astype(jnp.bfloat16)
                    n_buf[top:end, pl.ds(pl.multiple_of(r * size + k * head, head), head)] = jnp.dot(probs, qkv[vals, :end, cols], preferred_element_type=jnp.float32).astype(jnp.bfloat16)

    gathers[keys].forward()
    loads[queries].wait()
    gathers[queries].begin()
    gathers[vals].forward()
    complete(keys)
    project(keys, keep(keys))
    gathers[queries].forward()
    loads[outs].wait()
    gathers[outs].begin()
    complete(vals)
    project(vals, keep(vals))
    complete(queries)
    project(queries, keep(queries))
    attend(0, group // 2)
    gathers[outs].forward()
    attend(group // 2, group)
    gathers[outs].arrive(gathers[outs].mate + gathers[outs].near_mate)
    side = group // 2
    spans = [(r0 * size, (r0 + side - 1) * size) for r0 in (0, side)]

    @pl.loop(0, d_model // width)
    def _(c):
        cols = pl.ds(pl.multiple_of(c * width, width), width)
        weights = [jnp.concatenate([w_buf[outs, r, :, cols] for r in range(r0, r0 + side - 1)], axis=0) for r0 in (0, side)]
        parts = [jnp.dot(n_buf[:, lo:hi], weight, preferred_element_type=jnp.float32) for (lo, hi), weight in zip(spans, weights)]
        acc[:, cols] = parts[0] + parts[1]

    gathers[outs].forward_far()
    gathers[outs].arrive(gathers[outs].far_mate)

    @pl.loop(0, d_model // width)
    def _(c):
        cols = pl.ds(pl.multiple_of(c * width, width), width)
        parts = [jnp.dot(n_buf[:, hi:hi + size], w_buf[outs, hi // size, :, cols], preferred_element_type=jnp.float32) for lo, hi in spans]
        attn = (acc[:, cols] + parts[0] + parts[1]).astype(jnp.bfloat16)
        h_ref[:, cols] = (x_ref[:, cols].astype(jnp.float32) + attn.astype(jnp.float32)).astype(jnp.bfloat16)

    for r in range(group):
        ids_out[r] = ids_buf[r]
    for gather in gathers + [ids_gather]:
        gather.finish()


def attention_layer(x, ids_t, k_shard, v_shard, q_shard, o_shard, group, local):
    n_tok, d_model = x.shape
    top_k = ids_t.shape[0]
    vmem = pl.BlockSpec(memory_space=pltpu.VMEM)
    anywhere = pl.BlockSpec(memory_space=pl.ANY)
    return pl.pallas_call(
        attention_layer_kernel,
        in_specs=[vmem] + [anywhere] * 5,
        out_specs=[vmem] * 3,
        out_shape=[jax.ShapeDtypeStruct(x.shape, jnp.bfloat16), jax.ShapeDtypeStruct((group, local, n_tok), jnp.int32), jax.ShapeDtypeStruct((group, top_k, n_tok), jnp.int32)],
        scratch_shapes=[
            pltpu.VMEM((4, group) + k_shard.shape, jnp.bfloat16),
            pltpu.VMEM(x.shape, jnp.bfloat16),
            pltpu.VMEM((3,) + x.shape, jnp.bfloat16),
            pltpu.VMEM(x.shape, jnp.float32),
            pltpu.VMEM((group, top_k, n_tok), jnp.int32),
            pltpu.SemaphoreType.DMA((5,)),
            pltpu.SemaphoreType.DMA((4, 9)),
            pltpu.SemaphoreType.DMA((4, 9)),
            pltpu.SemaphoreType.DMA((9,)),
            pltpu.SemaphoreType.DMA((9,)),
        ],
        compiler_params=pltpu.CompilerParams(vmem_limit_bytes=MAX_VMEM, collective_id=0, has_side_effects=True),
        cost_estimate=pl.CostEstimate(flops=9 * n_tok * d_model * d_model, bytes_accessed=8 * d_model * d_model // group, transcendentals=0),
        name="attention_layer",
    )(x, ids_t, k_shard, v_shard, q_shard, o_shard)


def dispatch_kernel(h_ref, wr_ref, ids_ref, rank_ref, x_hbm, gates_ref, u_hbm, u_buf, pick, stage, g_buf, out_sems, send, recv, g_send, g_recv):
    n_tok, d_model = h_ref.shape
    group, local = rank_ref.shape[:2]
    capacity = x_hbm.shape[2]
    n_experts = wr_ref.shape[0]
    top_k = ids_ref.shape[0]
    width = stage.shape[3]
    n_cols = d_model // width
    tokens = Gather(u_buf, send, recv)
    gates = Gather(g_buf, g_send, g_recv, split=False)

    @pl.loop(0, n_tok // 128)
    def _(i):
        rows = pl.ds(pl.multiple_of(i * 128, 128), 128)
        u_buf[0, rows, :] = rms_norm(h_ref[rows, :]).astype(jnp.bfloat16)

    greet(neighbour(1), neighbour(-1), neighbour(2), neighbour(0, True))
    tokens.begin()
    keep = pltpu.make_async_copy(u_buf.at[0], u_hbm, out_sems.at[2])
    keep.start()

    for i in range(n_tok // 128):
        rows = slice(i * 128, (i + 1) * 128)
        logits = lax.dot_general(wr_ref[...], rms_norm(h_ref[rows, :]), (((1,), (1,)), ((), ())), precision=lax.Precision.HIGHEST, preferred_element_type=jnp.float32)
        experts_iota = lax.broadcasted_iota(jnp.int32, (n_experts, 128), 0)
        chosen = jnp.concatenate([jnp.sum(jnp.where(experts_iota == ids_ref[j:j + 1, rows], logits, 0.0), axis=0, keepdims=True) for j in range(top_k)], axis=0)
        weights = jnp.exp(chosen - jnp.max(chosen, axis=0, keepdims=True))
        g_buf[0, :, rows] = weights / jnp.sum(weights, axis=0, keepdims=True)
    gates.begin()

    def put(r, c, slot):
        cols = pl.ds(pl.multiple_of(c * width, width), width)
        return pltpu.make_async_copy(stage.at[slot], x_hbm.at[r, :, :, cols], out_sems.at[slot])

    def dispatch(r, before):
        slots = lax.broadcasted_iota(jnp.int32, (capacity, n_tok), 0)
        for e in range(local):
            pick[e * capacity:(e + 1) * capacity, :] = (rank_ref[r, e:e + 1, :] == slots).astype(jnp.float32).astype(jnp.bfloat16)

        @pl.loop(0, n_cols)
        def _(c):
            slot = lax.rem(c, 2)
            cols = pl.ds(pl.multiple_of(c * width, width), width)
            if before is None:
                @pl.when(c >= 2)
                def _():
                    put(r, c - 2, slot).wait()
            else:
                @pl.when(c >= 2)
                def _():
                    put(r, c - 2, slot).wait()

                @pl.when(c < 2)
                def _():
                    put(before, n_cols - 2 + c, slot).wait()
            rows = jnp.dot(pick[...], u_buf[r, :, cols], preferred_element_type=jnp.float32).astype(jnp.bfloat16)
            for e in range(local):
                stage[slot, e] = rows[e * capacity:(e + 1) * capacity, :]
            put(r, c, slot).start()

    dispatch(0, None)
    tokens.arrive(tokens.mate)
    dispatch(4, 0)
    tokens.forward()
    dispatch(1, 4)
    dispatch(2, 1)
    tokens.arrive(tokens.near_mate)
    dispatch(5, 2)
    dispatch(6, 5)
    tokens.forward_far()
    dispatch(3, 6)
    gates.arrive(gates.own + gates.mate)
    for copy in gates.near_mate:
        copy.start()
    gates.forward_far()
    tokens.arrive(tokens.far_mate)
    dispatch(7, 3)
    gates.arrive(gates.near_mate + gates.far_mate)
    for r in range(group):
        gates_ref[r] = g_buf[r]
    for c in range(n_cols - 2, n_cols):
        put(7, c, c % 2).wait()
    keep.wait()
    tokens.finish()
    gates.finish()


def dispatch_tokens(h, router_t, ids_t, rank, capacity):
    n_tok, d_model = h.shape
    group, local = rank.shape[:2]
    top_k = ids_t.shape[0]
    width = 512
    vmem = pl.BlockSpec(memory_space=pltpu.VMEM)
    return pl.pallas_call(
        dispatch_kernel,
        in_specs=[vmem] * 4,
        out_specs=[pl.BlockSpec(memory_space=pl.ANY), vmem, pl.BlockSpec(memory_space=pl.ANY)],
        out_shape=[jax.ShapeDtypeStruct((group, local, capacity, d_model), jnp.bfloat16), jax.ShapeDtypeStruct((group, top_k, n_tok), jnp.float32), jax.ShapeDtypeStruct(h.shape, jnp.bfloat16)],
        scratch_shapes=[
            pltpu.VMEM((group, n_tok, d_model), jnp.bfloat16),
            pltpu.VMEM((local * capacity, n_tok), jnp.bfloat16),
            pltpu.VMEM((2, local, capacity, width), jnp.bfloat16),
            pltpu.VMEM((group, top_k, n_tok), jnp.float32),
            pltpu.SemaphoreType.DMA((3,)),
            pltpu.SemaphoreType.DMA((9,)),
            pltpu.SemaphoreType.DMA((9,)),
            pltpu.SemaphoreType.DMA((9,)),
            pltpu.SemaphoreType.DMA((9,)),
        ],
        compiler_params=pltpu.CompilerParams(vmem_limit_bytes=MAX_VMEM, collective_id=1, has_side_effects=True),
        cost_estimate=pl.CostEstimate(flops=2 * group * local * capacity * n_tok * d_model, bytes_accessed=2 * group * local * capacity * d_model, transcendentals=0),
        name="dispatch_tokens",
    )(h, router_t, ids_t, rank)


def expert_kernel(size_ref, start_ref, total_ref, x_ref, gate_ref, up_ref, down_ref, f_ref, x_buf, f_buf, in_sems, out_sems, *, chunk):
    n_src, _, capacity, d_model = x_ref.shape
    e, local = pl.program_id(0), pl.num_programs(0)
    slot = lax.rem(e, 2)
    zeros = jnp.zeros((capacity, d_model), jnp.bfloat16)

    def fetch(r, expert, where):
        size = pl.multiple_of(size_ref[r, expert], ALIGN)
        start = pl.multiple_of(start_ref[r, expert], ALIGN)
        return pltpu.make_async_copy(x_ref.at[r, expert, pl.ds(0, size), :], x_buf.at[where, pl.ds(start, size), :], in_sems.at[where, r])

    def put(r, expert, where):
        start = pl.multiple_of(start_ref[r, expert], ALIGN)
        return pltpu.make_async_copy(f_buf.at[where, pl.ds(start, capacity), :], f_ref.at[r, expert], out_sems.at[where, r])

    @pl.when(e == 0)
    def _():
        for r in range(n_src):
            fetch(r, 0, 0).start()

    @pl.when(e + 1 < local)
    def _():
        for r in range(n_src):
            fetch(r, e + 1, 1 - slot).start()

    for r in range(n_src):
        fetch(r, e, slot).wait()

    @pl.when(e >= 2)
    def _():
        for r in range(n_src):
            put(r, e - 2, slot).wait()

    total = total_ref[e]
    x_buf[slot, pl.ds(pl.multiple_of(total, ALIGN), capacity), :] = zeros
    chunks = (total + chunk - 1) // chunk

    def run(start, size):
        rows = pl.ds(pl.multiple_of(start, chunk), size)
        x = x_buf[slot, rows, :]
        gate_act = jnp.dot(x, gate_ref[0], preferred_element_type=jnp.float32)
        up_act = jnp.dot(x, up_ref[0], preferred_element_type=jnp.float32)
        middle = (gate_act * jax.nn.sigmoid(gate_act) * up_act).astype(jnp.bfloat16)
        f_buf[slot, rows, :] = jnp.dot(middle, down_ref[0], preferred_element_type=jnp.float32).astype(jnp.bfloat16)

    @pl.loop(0, chunks // 2)
    def _(i):
        run(i * 2 * chunk, 2 * chunk)

    @pl.when(lax.rem(chunks, 2) == 1)
    def _():
        run((chunks - 1) * chunk, chunk)

    f_buf[slot, pl.ds(pl.multiple_of(chunks * chunk, chunk), capacity), :] = zeros
    for r in range(n_src):
        put(r, e, slot).start()

    @pl.when(e == local - 1)
    def _():
        @pl.when(e >= 1)
        def _():
            for r in range(n_src):
                put(r, e - 1, 1 - slot).wait()
        for r in range(n_src):
            put(r, e, slot).wait()


def experts(sizes, starts, totals, rows, gate_w, up_w, down_w):
    n_src, local, capacity, d_model = rows.shape
    width = gate_w.shape[2]
    chunk = capacity
    n_rows = n_src * capacity + 2 * capacity
    anywhere = pl.BlockSpec(memory_space=pl.ANY)
    return pl.pallas_call(
        functools.partial(expert_kernel, chunk=chunk),
        grid_spec=pltpu.PrefetchScalarGridSpec(
            num_scalar_prefetch=3,
            grid=(local,),
            in_specs=[anywhere] + [
                pl.BlockSpec((1, d_model, width), lambda e, *_: (e, 0, 0)),
                pl.BlockSpec((1, d_model, width), lambda e, *_: (e, 0, 0)),
                pl.BlockSpec((1, width, d_model), lambda e, *_: (e, 0, 0)),
            ],
            out_specs=anywhere,
            scratch_shapes=[
                pltpu.VMEM((2, n_rows, d_model), jnp.bfloat16),
                pltpu.VMEM((2, n_rows, d_model), jnp.bfloat16),
                pltpu.SemaphoreType.DMA((2, n_src)),
                pltpu.SemaphoreType.DMA((2, n_src)),
            ],
        ),
        out_shape=jax.ShapeDtypeStruct(rows.shape, jnp.bfloat16),
        compiler_params=params(),
        cost_estimate=pl.CostEstimate(flops=4 * local * n_src * capacity * d_model * width, bytes_accessed=6 * local * d_model * width, transcendentals=0),
        name="experts",
    )(sizes, starts, totals, rows, gate_w, up_w, down_w)


def reduce_kernel(rank_ref, ids_ref, gates_ref, f_ref, h_hbm, u_hbm, pair_hbm, down_hbm, out_ref, f_buf, spread, other_buf, swap_buf, send_buf, ring_buf, f_sems, swap_send, swap_recv, ring_send, ring_recv, out_sems, free_sem):
    n_src, local, n_tok = rank_ref.shape
    capacity = f_ref.shape[2]
    top_k = ids_ref.shape[1]
    pieces = spread.shape[1]
    chips = n_src // 2
    width = out_ref.shape[1] // 4
    n_units = 16

    def quarter(u):
        return 2 * lax.rem(u, 2) + u // 2

    def place(i):
        u = lax.rem(i, 4)
        odd = lax.rem(u, 2)
        target = jnp.where(i < 4, 1 + odd, jnp.where(i < 8, 2 - odd, jnp.where(i < 12, 3, 0)))
        return u, target

    def fetch(i, side, slot):
        u, target = place(i)
        cols = pl.ds(pl.multiple_of(quarter(u) * width, width), width)
        return pltpu.make_async_copy(f_ref.at[target + chips * (1 - side), :, :, cols], f_buf.at[slot, side], f_sems.at[slot, side])

    def swap_copy(i):
        s = lax.rem(i, 4)
        return remote(other_buf.at[s], swap_buf.at[s], swap_send.at[s], swap_recv.at[s], neighbour(0, True))

    def ring_copy(source, slot):
        return remote(send_buf.at[source], ring_buf.at[slot], ring_send.at[slot], ring_recv.at[slot], neighbour(1 - 2 * lax.rem(slot, 2)))

    def build(target, entry):
        @pl.loop(0, 2)
        def _(side):
            r = target + chips * (1 - side)
            first = lax.axis_index('ep') * local
            ids = ids_ref[r]
            gates = gates_ref[r]
            rest = jnp.concatenate([jnp.sum(jnp.where(ids == first + e, gates, 0.0), axis=0, keepdims=True) for e in range(local)], axis=0)
            table = [rank_ref[r].astype(jnp.float32)]
            for _ in range(pieces):
                table.append(rest.astype(jnp.bfloat16).astype(jnp.float32))
                rest = rest - table[-1]
            table = jnp.concatenate(table, axis=0).T
            rank = table[:, :local].astype(jnp.int32)
            weights = table[:, local:]
            slots = lax.broadcasted_iota(jnp.int32, (n_tok, capacity), 1)
            for e in range(local):
                hit = rank[:, e:e + 1] == slots
                for k in range(pieces):
                    column = k * local + e
                    spread[entry * 2 + side, k, :, e * capacity:(e + 1) * capacity] = jnp.where(hit, weights[:, column:column + 1], 0.0).astype(jnp.bfloat16)

    def product(entry, slot, side):
        data = jnp.concatenate([f_buf[slot, side, e] for e in range(local)], axis=0)
        total = jnp.dot(spread[entry * 2 + side, 0], data, preferred_element_type=jnp.float32)
        for k in range(1, pieces):
            total += jnp.dot(spread[entry * 2 + side, k], data, preferred_element_type=jnp.float32)
        return total

    for side in range(2):
        fetch(0, side, 0).start()
    greet(neighbour(1), neighbour(-1), neighbour(0, True))

    @pl.loop(0, n_units)
    def _(i):
        u, target = place(i)
        slot = lax.rem(i, 2)
        lane = lax.rem(i, 4)

        @pl.when(i + 1 < n_units)
        def _():
            for side in range(2):
                fetch(i + 1, side, 1 - slot).start()

        @pl.when(i == 0)
        def _():
            build(1, 0)

        @pl.when(i == 1)
        def _():
            build(2, 1)

        @pl.when(i == 8)
        def _():
            build(3, 0)

        @pl.when(i == 12)
        def _():
            build(0, 1)

        entry = 1 - lax.rem(target, 2)

        @pl.when(i >= 4)
        def _():
            swap_copy(i - 4).wait_send()
            pl.semaphore_wait(free_sem, 1)

        fetch(i, 0, slot).wait()
        other_buf[lane] = product(entry, slot, 0)
        swap_copy(i).start()
        fetch(i, 1, slot).wait()
        send_buf[i] = product(entry, slot, 1)
        swap_copy(i).wait_recv()
        send_buf[i] += swap_buf[lane]

        @pl.when(i < n_units - 4)
        def _():
            pl.semaphore_signal(free_sem, inc=1, device_id=neighbour(0, True), device_id_type=pl.DeviceIdType.MESH)

        @pl.when(i < 4)
        def _():
            ring_copy(i, u).start()

        @pl.when((i >= 8) & (i < 12))
        def _():
            ring_copy(i, u).wait_recv()
            send_buf[i] += ring_buf[u]
            ring_copy(i, u + 4).start()

    @pl.loop(0, 4)
    def _(u):
        ring_copy(0, u + 4).wait_recv()
        send_buf[u + 4] += ring_buf[u + 4]
        ring_copy(u + 4, u + 8).start()

    for u in range(4):
        swap_copy(n_units - 4 + u).wait_send()
    half = 2 * width
    loads = []
    for k in range(2):
        cols = pl.ds(k * half, half)
        loads.append(pltpu.make_async_copy(u_hbm.at[:, cols], spread.at[0, 1 + k], out_sems.at[k]))
        loads.append(pltpu.make_async_copy(h_hbm.at[:, cols], spread.at[1, k], out_sems.at[2 + k]))

    def shared_tile(t, side):
        slot = lax.rem(t, 2)
        depth = pl.ds(pl.multiple_of(lax.rem(t, 2) * local, local), local)
        cols = pl.ds(pl.multiple_of((t // 2 + 2 * side) * width, width), width)
        return pltpu.make_async_copy(pair_hbm.at[depth, :, cols], f_buf.at[slot, side], f_sems.at[slot, side])

    def down_tile(q):
        slot = lax.rem(q, 2)
        cols = pl.ds(pl.multiple_of(q * width, width), width)
        return pltpu.make_async_copy(down_hbm.at[:, :, cols], f_buf.at[slot, 0], f_sems.at[slot, 0])

    for load in loads:
        load.start()
    for side in range(2):
        shared_tile(0, side).start()
    for load in loads:
        load.wait()

    @pl.loop(0, 4)
    def _(t):
        @pl.when(t < 3)
        def _():
            for side in range(2):
                shared_tile(t + 1, side).start()

        @pl.when(t == 3)
        def _():
            down_tile(0).start()

        k = lax.rem(t, 2)
        for side in range(2):
            shared_tile(t, side).wait()
            data = jnp.concatenate([f_buf[k, side, e] for e in range(local)], axis=0)
            part = jnp.dot(spread[0, 1 + k], data, preferred_element_type=jnp.float32)

            @pl.when(k == 0)
            def _():
                other_buf[side] = part

            @pl.when(k == 1)
            def _():
                other_buf[side] += part

        @pl.when(k == 1)
        def _():
            gate_act = other_buf[0]
            middle = gate_act * jax.nn.sigmoid(gate_act) * other_buf[1]
            spread[0, 0, :, pl.ds(pl.multiple_of(t // 2 * width, width), width)] = middle.astype(jnp.bfloat16)

    @pl.loop(0, 4)
    def _(q):
        @pl.when(q < 3)
        def _():
            down_tile(q + 1).start()

        down_tile(q).wait()
        data = jnp.concatenate([f_buf[lax.rem(q, 2), 0, e] for e in range(local)], axis=0)
        swap_buf[q] = jnp.dot(spread[0, 0], data, preferred_element_type=jnp.float32).astype(jnp.bfloat16).astype(jnp.float32)

    def put(u):
        q = quarter(u)
        inner = pl.ds(pl.multiple_of(lax.rem(q, 2) * width, width), width)
        cols = pl.ds(pl.multiple_of(q * width, width), width)
        return pltpu.make_async_copy(spread.at[3, q // 2, :, inner], out_ref.at[:, cols], out_sems.at[u])

    @pl.loop(0, 4)
    def _(u):
        q = quarter(u)
        inner = pl.ds(pl.multiple_of(lax.rem(q, 2) * width, width), width)
        ring_copy(0, u + 8).wait_recv()
        routed = send_buf[12 + u] + ring_buf[u + 8]
        spread[3, q // 2, :, inner] = (spread[1, q // 2, :, inner].astype(jnp.float32) + routed + swap_buf[q]).astype(jnp.bfloat16)
        put(u).start()

    @pl.loop(0, 4)
    def _(u):
        put(u).wait()
        ring_copy(u, u).wait_send()
        ring_copy(8 + u, u + 4).wait_send()
        ring_copy(4 + u, u + 8).wait_send()


def reduce_results(rank, ids, gates, results, residual, moe_in, pair_w, down_w):
    n_src, local, capacity, d_model = results.shape
    n_tok = rank.shape[2]
    width = d_model // 4
    n_pieces = 3
    tile = (n_tok, width)
    vmem = pl.BlockSpec(memory_space=pltpu.VMEM)
    return pl.pallas_call(
        reduce_kernel,
        in_specs=[vmem] * 3 + [pl.BlockSpec(memory_space=pl.ANY)] * 5,
        out_specs=pl.BlockSpec(memory_space=pl.ANY),
        out_shape=jax.ShapeDtypeStruct((n_tok, d_model), jnp.bfloat16),
        scratch_shapes=[
            pltpu.VMEM((2, 2, local, capacity, width), jnp.bfloat16),
            pltpu.VMEM((4, n_pieces, n_tok, local * capacity), jnp.bfloat16),
            pltpu.VMEM((4,) + tile, jnp.float32),
            pltpu.VMEM((4,) + tile, jnp.float32),
            pltpu.VMEM((16,) + tile, jnp.float32),
            pltpu.VMEM((12,) + tile, jnp.float32),
            pltpu.SemaphoreType.DMA((2, 2)),
            pltpu.SemaphoreType.DMA((4,)),
            pltpu.SemaphoreType.DMA((4,)),
            pltpu.SemaphoreType.DMA((12,)),
            pltpu.SemaphoreType.DMA((12,)),
            pltpu.SemaphoreType.DMA((4,)),
            pltpu.SemaphoreType.REGULAR,
        ],
        compiler_params=pltpu.CompilerParams(vmem_limit_bytes=MAX_VMEM, collective_id=2, has_side_effects=True),
        cost_estimate=pl.CostEstimate(flops=6 * n_src * local * capacity * n_tok * d_model, bytes_accessed=4 * n_src * local * capacity * d_model, transcendentals=0),
        name="reduce_results",
    )(rank, ids, gates, results, residual, moe_in, *[w.reshape(-1, capacity, w.shape[1]) for w in (pair_w, down_w)])


def local_layer(x_loc, q_shard, k_shard, v_shard, o_shard, w_router, gate_loc, up_loc, down_loc, sgate_shard, sup_shard, sdown_shard, ids_loc, group):
    n_seq, seq_len, d_model = x_loc.shape
    assert n_seq == 1 and group == 8 and q_shard.shape[2] == 128
    n_tok = n_seq * seq_len
    top_k = ids_loc.shape[-1]
    local = gate_loc.shape[0]
    n_experts = local * group
    capacity = CAP_FACTOR * n_tok * top_k // n_experts
    def gathered(shard):
        return lax.all_gather(shard.reshape(shard.shape[0], -1), 'ep', axis=0, tiled=True)

    x_flat = x_loc.reshape(n_tok, d_model)
    ids_t = ids_loc.reshape(n_tok, top_k).T
    residual, rank, ids_all = attention_layer(x_flat, ids_t, *[w.reshape(w.shape[0], -1) for w in (k_shard, v_shard, q_shard, o_shard)], group, local)
    rows, gates_all, moe_in = dispatch_tokens(residual, w_router.T, ids_t, rank, capacity)

    sizes = (jnp.max(rank, axis=2) + 1 + ALIGN - 1) // ALIGN * ALIGN
    ends = jnp.cumsum(sizes, axis=0)
    starts, totals = ends - sizes, ends[-1]
    pair_shard = jnp.concatenate([sgate_shard, sup_shard], axis=1)
    rows, pair_shard, sdown_shard = lax.optimization_barrier((rows, pair_shard, sdown_shard))
    results = experts(sizes, starts, totals, rows, gate_loc, up_loc, down_loc)

    y_out = reduce_results(rank, ids_all, gates_all, results, residual, moe_in, gathered(pair_shard), gathered(sdown_shard))
    return y_out.reshape(n_seq, seq_len, d_model)


def solution(mesh):
    tok_spec = P(('dp', 'ep'), None, None)
    row_spec = P('ep', None)
    cube_spec = P('ep', None, None)
    in_specs = (tok_spec, cube_spec, cube_spec, cube_spec, row_spec, P(None, None), cube_spec, cube_spec, cube_spec, row_spec, row_spec, row_spec, tok_spec)
    return jax.shard_map(functools.partial(local_layer, group=mesh.shape['ep']), mesh=mesh, in_specs=in_specs, out_specs=tok_spec, check_vma=False)
```
